32 devices in a mesh: gx: 4 (over y, x), gy: 8 (over z, core).
Axes of the slice: x: 2, y: 2, z: 4, core: 2. Of those that a mesh axis runs over, the one named last changes fastest.
Arguments:
- populations: float32 [19, 128, 64, 256], P(None, 'gx', 'gy'), may hold values from 0.02 to 0.08
- mass: float32 [256, 1024], P('gx', 'gy'), may hold values from 0.2 to 1
- modulus: float32 [256, 1024], P('gx', 'gy'), may hold values from 0.1 to 0.5
- cell_live: int32 [256, 1024], P('gx', 'gy'), may hold values 0 or 1
- stiff_ref: float32 [12, 12], replicated, as said below
- rec_block: int32 [131072], P(('gx', 'gy')), may hold values from 0 to 255
- rec_owner: int32 [131072, 1], P(('gx', 'gy')), may hold values from 0 to 31; in each aligned block of 4096 rows (0 to 4095, 4096 to 8191, ...) at most 256 rows name the same one
- rec_node: int32 [131072], P(('gx', 'gy')), may hold values from 0 to 8191
- rbf_weight: float32 [131072, 256], P(('gx', 'gy')), may hold values from 0 to 2
Outputs:
- populations_next: float32 [19, 128, 64, 256], P(None, 'gx', 'gy')
- displacement: float32 [3, 256, 1024], P(None, 'gx', 'gy')
The draws below stay inside these ranges and needn't reach their ends.
Inputs may be any that keep to these rules, and one draw needn't show every extreme that they name: `rec_owner`: in the records of one device no owner is named more than 256 times, and every owner is named by some record. `stiff_ref`: symmetric with a positive diagonal that exceeds the sum of magnitudes of each row's other entries.
All inputs are finite; a program needn't handle non-finite values. No bound on the sum of `cell_live` on one device may be relied on, other than what follows from the above.
Results may differ from the reference program's by a relative error of at most 0.0003.
Values sent between devices are 32-bit elements; how exact they have to be, the bound alone decides.
A program may use at most 128 MiB of HBM per device.

```python
import math
import jax
import jax.numpy as jnp
import numpy as np
from jax import lax

CX = 32
CY = 8
CZ = 256
PU = 64
PV = 128
R_DEV = 4096
ITERS = 2
NX = 128
NY = 64
NZ = 256
NU = 256
NV = 1024
CAP = 256
R_TOTAL = 131072
N_GX = 4
N_GY = 8
DEVICES = 32


def draw_stiff_ref(key, part):
    first_key, second_key = jax.random.split(jax.random.fold_in(key, 17))
    offdiag = jax.random.uniform(first_key, (12, 12), jnp.float32, -0.3, 0.3)
    offdiag = (offdiag + offdiag.T) * 0.5 * (1.0 - jnp.eye(12, dtype=jnp.float32))
    diagonal = jnp.sum(jnp.abs(offdiag), axis=1) + jax.random.uniform(second_key, (12,), jnp.float32, 0.3, 0.8)
    return offdiag + jnp.diag(diagonal)


def plant(values, rng, smallest, top_value):
    extent = values.shape
    index_at = [jax.random.randint(jax.random.fold_in(rng, axis), (), 0, extent[axis]) for axis in range(len(extent))]
    values = values.at[tuple(index_at)].set(smallest)
    longest = extent.index(max(extent))
    index_at[longest] = (index_at[longest] + 1) % extent[longest]
    return values.at[tuple(index_at)].set(top_value)


def steps_of(stream_key, extent, pieces, low, high):
    gain = 1.0
    for axis_at, parts in pieces:
        draws = jax.random.uniform(jax.random.fold_in(jax.random.fold_in(stream_key, 6), axis_at), (parts,), jnp.float32, low / len(pieces), high / len(pieces))
        gain = gain * jnp.repeat(jnp.exp(draws), extent[axis_at] // parts).reshape((-1,) + (1,) * (len(extent) - 1 - axis_at))
    return gain


def deal_out(own_key, own, number, rows, number_of, top, bound, slope):
    order = jax.random.permutation(own_key, number_of)
    crowded, common = portions_of(number_of, rows * top, bound, slope, True), portions_of(number_of, rows * top, bound, slope, False)
    places = jnp.arange(number_of)

    def named(tallies, rotation):
        used = int((tallies > 0).sum())
        fixed = max(1, used // 4)
        moved = fixed + (places - fixed + rotation * (used - fixed)) % max(1, number_of - fixed)
        return jnp.zeros((number_of,), jnp.int32).at[order[jnp.where(places < fixed, places, moved)]].set(jnp.asarray(tallies, jnp.int32))

    tallies = jnp.where(number % 4 == 0, named(crowded, number // 4), named(common, number - number // 4 - 1))
    mixed = jax.random.permutation(jax.random.fold_in(own, 3), number_of)
    donor, taker = mixed[0:number_of // 2 * 2:2], mixed[1:number_of // 2 * 2:2]
    slack = jnp.minimum(tallies[donor] - 1, bound - tallies[taker]) // 2
    slack = jnp.where((donor == order[0]) | (taker == order[0]) | (tallies[taker] == 0), 0, jnp.maximum(slack, 0))
    moved = jax.random.randint(jax.random.fold_in(own, 4), (number_of // 2,), 0, 1 << 20) % (slack + 1)
    tallies = tallies.at[donor].add(-moved).at[taker].add(moved)
    members = jnp.searchsorted(jnp.cumsum(tallies), jnp.arange(rows * top), side="right").astype(jnp.int32)
    grid = members.reshape(top, rows).T
    grid = grid[jax.random.permutation(jax.random.fold_in(own, 1), rows)]
    rotation = jax.random.randint(jax.random.fold_in(own, 2), (rows, 1), 0, top)
    return jnp.take_along_axis(grid, (jnp.arange(top)[None, :] + rotation) % top, axis=1)


def portions_of(amount, total, reach, lean, full):
    portions = [(1 << 20) // math.isqrt(standing ** lean) + 1 for standing in range(1, amount + 1)]
    largest = reach if full else min(reach, max(-(-total // amount), total * portions[0] // sum(portions)))
    least = 1 if total - largest >= amount - 1 else 0
    holding, rest = [largest] + [least] * (amount - 1), total - largest - least * (amount - 1)
    while rest > 0:
        movable = [i for i in range(1, amount) if holding[i] < largest] or [i for i in range(1, amount) if holding[i] < reach]
        pool, budget = sum([portions[i] for i in movable]), rest
        for i in movable:
            extra = min(reach - holding[i], max(1, budget * portions[i] // pool), rest)
            holding[i] = holding[i] + extra
            rest = rest - extra
    return np.array(holding)


def setup_inputs(seed: int = 0) -> dict:
    seeds = jax.random.split(jax.random.key(seed), 10)
    populations = jnp.clip(0.02 + 0.06 * jax.random.uniform(seeds[0], (19, NX, NY, NZ), jnp.float32) ** steps_of(seeds[0], (19, NX, NY, NZ), ((1, 4), (2, 8)), -0.2, 0.2), 0.02, 0.08)
    mass = jnp.clip(jnp.exp(math.log(1.0) - 1.609438 * jax.random.uniform(seeds[1], (NU, NV), jnp.float32) ** steps_of(seeds[1], (NU, NV), ((0, 4), (1, 8)), -0.2, 0.2)), 0.2, 1.0)
    modulus = jnp.clip(jnp.exp(math.log(0.5) - 1.609438 * jax.random.uniform(seeds[2], (NU, NV), jnp.float32) ** steps_of(seeds[2], (NU, NV), ((0, 4), (1, 8)), -0.2, 0.2)), 0.1, 0.5)
    cell_live = plant((jax.random.randint(seeds[3], (NU, NV), 0, 8) < 7).astype(jnp.int32), jax.random.fold_in(seeds[3], 1), 0, 1)
    stiff_ref = draw_stiff_ref(jax.random.fold_in(seeds[9], 71), 0)
    rec_block = plant(jax.random.randint(seeds[5], (R_TOTAL,), 0, CX * CY), jax.random.fold_in(seeds[5], 1), 0, (CX * CY) - 1).astype(jnp.int32)
    rec_owner_keys = jax.random.split(jax.random.fold_in(seeds[6], 1), R_TOTAL // R_DEV)
    rec_owner_turns = jax.random.permutation(jax.random.fold_in(seeds[6], 3), R_TOTAL // R_DEV)
    rec_owner = jax.vmap(lambda own, number: deal_out(jax.random.fold_in(seeds[6], 2), own, number, R_DEV, DEVICES, 1, CAP, 2))(rec_owner_keys, rec_owner_turns).reshape((R_TOTAL, 1))
    rec_node = plant(jax.random.randint(seeds[7], (R_TOTAL,), 0, PU * PV), jax.random.fold_in(seeds[7], 1), 0, (PU * PV) - 1).astype(jnp.int32)
    rbf_weight = jnp.clip(2.0 * jax.random.uniform(seeds[8], (R_TOTAL, CZ), jnp.float32) ** steps_of(seeds[8], (R_TOTAL, CZ), ((0, 32),), -0.2, 0.2), 0.0, 2.0)
    return {"populations": populations, "mass": mass, "modulus": modulus, "cell_live": cell_live, "stiff_ref": stiff_ref, "rec_block": rec_block, "rec_owner": rec_owner, "rec_node": rec_node, "rbf_weight": rbf_weight}


lattice_dirs = ((0, 0, 0), (1, 0, 0), (-1, 0, 0), (0, 1, 0), (0, -1, 0), (0, 0, 1), (0, 0, -1),
                (1, 1, 0), (-1, -1, 0), (1, -1, 0), (-1, 1, 0), (1, 0, 1), (-1, 0, -1), (1, 0, -1),
                (-1, 0, 1), (0, 1, 1), (0, -1, -1), (0, 1, -1), (0, -1, 1))
lattice_weights = (1.0 / 3.0,) + (1.0 / 18.0,) * 6 + (1.0 / 36.0,) * 12
relax_rate = 1.25
coupling = 0.1


def combine_dirs(fields, direction):
    total = None
    for axis_pos in range(3):
        if direction[axis_pos] != 0:
            term = direction[axis_pos] * fields[axis_pos]
            total = term if total is None else total + term
    return total


def collide(populations):
    density = populations[0]
    for number in range(1, 19):
        density = density + populations[number]
    moment = []
    for axis_pos in range(3):
        total = None
        for number in range(19):
            if lattice_dirs[number][axis_pos] != 0:
                term = lattice_dirs[number][axis_pos] * populations[number]
                total = term if total is None else total + term
        moment.append(total)
    velocity = [moment[axis_pos] / density for axis_pos in range(3)]
    squared = velocity[0] * velocity[0] + velocity[1] * velocity[1] + velocity[2] * velocity[2]
    relaxed = []
    for number in range(19):
        projected = combine_dirs(velocity, lattice_dirs[number])
        if projected is None:
            bracket = 1.0 - 1.5 * squared
        else:
            bracket = 1.0 + 3.0 * projected + 4.5 * projected * projected - 1.5 * squared
        equilibrium = lattice_weights[number] * density * bracket
        relaxed.append(populations[number] - relax_rate * (populations[number] - equilibrium))
    return jnp.stack(relaxed), jnp.stack(moment)


def apply_forcing(read, forcing):
    result = []
    for number in range(19):
        projected = combine_dirs(forcing, lattice_dirs[number])
        if projected is None:
            result.append(read[number])
        else:
            result.append(read[number] + 3.0 * lattice_weights[number] * projected)
    return jnp.stack(result)


def stiffness(field, scale, stiff_ref):
    corners = jnp.concatenate([field, jnp.roll(field, -1, 1), jnp.roll(field, -1, 2),
                               jnp.roll(jnp.roll(field, -1, 1), -1, 2)], 0)
    result = scale[None] * jnp.einsum('kl,lab->kab', stiff_ref, corners, precision=lax.Precision.HIGHEST)
    return (result[0:3] + jnp.roll(result[3:6], 1, 1) + jnp.roll(result[6:9], 1, 2)
            + jnp.roll(jnp.roll(result[9:12], 1, 1), 1, 2))


def reference(populations, mass, modulus, cell_live, stiff_ref, rec_block, rec_owner, rec_node, rbf_weight):
    relaxed, moment = collide(populations)
    read = jnp.stack([jnp.roll(relaxed[number], lattice_dirs[number], axis=(0, 1, 2)) for number in range(19)])
    blocks_all = moment.reshape(3, N_GX, CX, N_GY, CY, NZ).transpose(1, 3, 0, 2, 4, 5).reshape(DEVICES, 3, CX * CY, NZ)
    block_dev = rec_block.reshape(DEVICES, R_DEV)
    kernel_dev = rbf_weight.reshape(DEVICES, R_DEV, CZ)

    def interpolate(packed):
        blocks, chosen, kernel = packed
        picked = blocks[:, chosen, :]
        return jnp.sum(picked * kernel[None], axis=2)

    loads = lax.map(interpolate, (blocks_all, block_dev, kernel_dev))
    loads_flat = loads.transpose(1, 0, 2).reshape(3, R_TOTAL)
    owners = rec_owner[:, 0]
    owner_x = owners // N_GY
    owner_y = owners % N_GY
    target = (owner_x * PU + rec_node // PV) * NV + owner_y * PV + rec_node % PV
    force = jax.ops.segment_sum(loads_flat.T, target, num_segments=NU * NV).T.reshape(3, NU, NV)
    scale = cell_live.astype(jnp.float32) * (modulus + jnp.roll(modulus, -1, 0) + jnp.roll(modulus, -1, 1)
                                             + jnp.roll(jnp.roll(modulus, -1, 0), -1, 1)) * 0.25

    def operate(field):
        return mass[None] * field + stiffness(field, scale, stiff_ref)

    displacement = jnp.zeros((3, NU, NV), jnp.float32)
    residual = force
    direction = force
    norm_now = jnp.sum(residual * residual)
    for step in range(ITERS):
        image = operate(direction)
        step_size = norm_now / jnp.sum(direction * image)
        displacement = displacement + step_size * direction
        residual = residual - step_size * image
        if step + 1 < ITERS:
            norm_next = jnp.sum(residual * residual)
            direction = residual + (norm_next / norm_now) * direction
            norm_now = norm_next
    moved = displacement.reshape(3, NU * NV)[:, target]
    moved_dev = moved.reshape(3, DEVICES, R_DEV).transpose(1, 0, 2)

    def spread(packed):
        chosen, kernel, shifted = packed
        empty = jnp.zeros((3, CX * CY, CZ), jnp.float32)
        return empty.at[:, chosen, :].add(coupling * kernel[None] * shifted[:, :, None])

    forcing = lax.map(spread, (block_dev, kernel_dev, moved_dev))
    forcing = forcing.reshape(N_GX, N_GY, 3, CX, CY, NZ).transpose(2, 0, 3, 1, 4, 5).reshape(3, NX, NY, NZ)
    return apply_forcing(read, forcing), displacement
```

```python
import functools
import math

import jax
import jax.numpy as jnp
from jax import lax
from jax.experimental import pallas as pl
from jax.experimental.pallas import tpu as pltpu
from jax.sharding import PartitionSpec as P

MESH = pl.DeviceIdType.MESH
F32 = jnp.float32
BF16 = jnp.bfloat16
LANES = 128

lattice_dirs = (
    (0, 0, 0),
    (1, 0, 0),
    (-1, 0, 0),
    (0, 1, 0),
    (0, -1, 0),
    (0, 0, 1),
    (0, 0, -1),
    (1, 1, 0),
    (-1, -1, 0),
    (1, -1, 0),
    (-1, 1, 0),
    (1, 0, 1),
    (-1, 0, -1),
    (1, 0, -1),
    (-1, 0, 1),
    (0, 1, 1),
    (0, -1, -1),
    (0, 1, -1),
    (0, -1, 1),
)
lattice_weights = (1.0 / 3.0,) + (1.0 / 18.0,) * 6 + (1.0 / 36.0,) * 12
relax_rate = 1.25
coupling = 0.1

x_up = [q for q in range(19) if lattice_dirs[q][0] == 1]
x_down = [q for q in range(19) if lattice_dirs[q][0] == -1]
y_up = [q for q in range(19) if lattice_dirs[q][1] == 1]
y_down = [q for q in range(19) if lattice_dirs[q][1] == -1]
diagonal = [q for q in range(19) if lattice_dirs[q][0] != 0 and lattice_dirs[q][1] != 0]


def combine_dirs(fields, direction):
    total = None
    for axis_pos in range(3):
        if direction[axis_pos] != 0:
            field = fields[axis_pos]
            if total is None:
                total = field if direction[axis_pos] == 1 else -field
            else:
                total = total + field if direction[axis_pos] == 1 else total - field
    return total


def halves(values):
    high = values.astype(BF16)
    low = (values - high.astype(F32)).astype(BF16)
    return high, low


def iota(shape, dim):
    return lax.broadcasted_iota(jnp.int32, shape, dim)


def dot_nt(left, right):
    return lax.dot_general(left, right, (((1,), (1,)), ((), ())), preferred_element_type=F32)


def dot_nn(left, right):
    return lax.dot_general(left, right, (((1,), (0,)), ((), ())), preferred_element_type=F32)


def collide_kernel(pop_ref, relaxed_ref, moment_ref, xu_ref, xd_ref, yu_ref, yd_ref):
    step = pl.program_id(0)
    last = pl.num_programs(0) - 1
    rows, cols, depth = pop_ref.shape[1:]

    def one(row, carry):
        pops = [pop_ref[q, row] for q in range(19)]
        density = pops[0]
        for q in range(1, 19):
            density = density + pops[q]
        moment = []
        for axis_pos in range(3):
            total = None
            for q in range(19):
                sign = lattice_dirs[q][axis_pos]
                if sign == 1:
                    total = pops[q] if total is None else total + pops[q]
                elif sign == -1:
                    total = -pops[q] if total is None else total - pops[q]
            moment.append(total)
            moment_ref[axis_pos, row] = total
        velocity = [moment[axis_pos] / density for axis_pos in range(3)]
        squared = (
            velocity[0] * velocity[0] + velocity[1] * velocity[1] + velocity[2] * velocity[2]
        )
        rest = 1.0 - 1.5 * squared
        for q in range(19):
            projected = combine_dirs(velocity, lattice_dirs[q])
            bracket = rest
            if projected is not None:
                bracket = rest + projected * (3.0 + 4.5 * projected)
            relaxed = (1.0 - relax_rate) * pops[q] + (
                relax_rate * lattice_weights[q]
            ) * density * bracket
            relaxed_ref[q, row] = relaxed
            if q in y_up:
                yu_ref[y_up.index(q), row] = relaxed[cols - 1 : cols]
            if q in y_down:
                yd_ref[y_down.index(q), row] = relaxed[0:1]
        return carry

    lax.fori_loop(0, rows, one, 0, unroll=2)

    @pl.when(step == 0)
    def _():
        for k, q in enumerate(x_down):
            xd_ref[k] = relaxed_ref[q, 0]

    @pl.when(step == last)
    def _():
        for k, q in enumerate(x_up):
            xu_ref[k] = relaxed_ref[q, rows - 1]


def collide(populations):
    _, nx, ny, nz = populations.shape
    rows = 8
    steps = nx // rows
    return pl.pallas_call(
        collide_kernel,
        grid=(steps,),
        in_specs=[pl.BlockSpec((19, rows, ny, nz), lambda i: (0, i, 0, 0))],
        out_specs=[
            pl.BlockSpec((19, rows, ny, nz), lambda i: (0, i, 0, 0)),
            pl.BlockSpec((3, rows, ny, nz), lambda i: (0, i, 0, 0)),
            pl.BlockSpec((5, ny, nz), lambda i: (0, 0, 0)),
            pl.BlockSpec((5, ny, nz), lambda i: (0, 0, 0)),
            pl.BlockSpec((5, rows, 1, nz), lambda i: (0, i, 0, 0)),
            pl.BlockSpec((5, rows, 1, nz), lambda i: (0, i, 0, 0)),
        ],
        out_shape=[
            jax.ShapeDtypeStruct((19, nx, ny, nz), F32),
            jax.ShapeDtypeStruct((3, nx, ny, nz), F32),
            jax.ShapeDtypeStruct((5, ny, nz), F32),
            jax.ShapeDtypeStruct((5, ny, nz), F32),
            jax.ShapeDtypeStruct((5, nx, 1, nz), F32),
            jax.ShapeDtypeStruct((5, nx, 1, nz), F32),
        ],
        compiler_params=pltpu.CompilerParams(dimension_semantics=("arbitrary",)),
        name="collide",
    )(populations)


def pack_kernel(
    devices, parts, node_cols, mom_ref, w_ref, blk_ref, own_ref, node_ref,
    out_ref, slot_ref, mom_cat, tri, base, acc,
):
    step = pl.program_id(0)
    blocks = mom_ref.shape[0] // 3
    chunk = w_ref.shape[0]

    @pl.when(step == 0)
    def _():
        high, low = halves(mom_ref[...])
        mom_cat[...] = jnp.concatenate([high, low, high], axis=1)
        before = iota((chunk, chunk), 0) <= iota((chunk, chunk), 1)
        tri[...] = before.astype(F32).astype(BF16)
        base[...] = jnp.zeros_like(base)
        acc[...] = jnp.zeros_like(acc)

    w_high, w_low = halves(w_ref[...])
    products = dot_nt(mom_cat[...], jnp.concatenate([w_high, w_high, w_low], axis=1))
    here = iota((blocks, chunk), 0) == blk_ref[...]
    loads = [
        jnp.sum(
            jnp.where(here, products[c * blocks : (c + 1) * blocks], 0.0), axis=0, keepdims=True
        )
        for c in range(3)
    ]
    owners = own_ref[...]
    hits = (iota((devices, chunk), 0) == owners).astype(F32)
    counts = dot_nn(hits.astype(BF16), tri[...])
    slots = jnp.sum(hits * (counts - 1.0 + base[:, 0:1]), axis=0, keepdims=True)
    base[...] = base[...] + counts[:, chunk - 1 : chunk]
    slot_id = slots.astype(jnp.int32)
    slot_ref[...] = slot_id
    part = slot_id // LANES
    place = slot_id - part * LANES
    node = node_ref[...]
    node_row = node // node_cols
    node_high = (node_row * node_cols).astype(F32)
    node_low = (node - node_row * node_cols).astype(F32)
    channel = iota((8, chunk), 0) // parts
    in_part = (iota((8, chunk), 0) - channel * parts) == part
    high_rows = jnp.zeros((8, chunk), F32)
    low_rows = jnp.zeros((8, chunk), F32)
    for c in range(4):
        if c < 3:
            high = loads[c].astype(BF16).astype(F32)
            low = loads[c] - high
        else:
            high, low = node_high, node_low
        high_rows = jnp.where(in_part & (channel == c), high, high_rows)
        low_rows = jnp.where(in_part & (channel == c), low, low_rows)
    mine = (iota((devices * 8, chunk), 0) // 8) == owners

    def spread(rows):
        tiled = jnp.broadcast_to(rows[None], (devices, 8, chunk)).reshape(devices * 8, chunk)
        return jnp.where(mine, tiled, 0.0).astype(BF16)

    slot_hot = (iota((LANES, chunk), 0) == place).astype(F32).astype(BF16)
    acc[...] += dot_nt(
        jnp.concatenate([spread(high_rows), spread(low_rows)], axis=1),
        jnp.concatenate([slot_hot, slot_hot], axis=1),
    )

    @pl.when(step == pl.num_programs(0) - 1)
    def _():
        out_ref[...] = acc[...].reshape(devices, 8, LANES)


def pack_loads(devices, parts, node_cols, moment, weights, blk, own, node):
    records, depth = weights.shape
    chunk = 512
    rows3 = moment.shape[0]
    row_spec = pl.BlockSpec((1, chunk), lambda i: (0, i))
    return pl.pallas_call(
        functools.partial(pack_kernel, devices, parts, node_cols),
        grid=(records // chunk,),
        in_specs=[
            pl.BlockSpec((rows3, depth), lambda i: (0, 0)),
            pl.BlockSpec((chunk, depth), lambda i: (i, 0)),
            row_spec,
            row_spec,
            row_spec,
        ],
        out_specs=[
            pl.BlockSpec((devices, 8, LANES), lambda i: (0, 0, 0)),
            row_spec,
        ],
        out_shape=[
            jax.ShapeDtypeStruct((devices, 8, LANES), F32),
            jax.ShapeDtypeStruct((1, records), jnp.int32),
        ],
        scratch_shapes=[
            pltpu.VMEM((rows3, 3 * depth), BF16),
            pltpu.VMEM((chunk, chunk), BF16),
            pltpu.VMEM((devices, LANES), F32),
            pltpu.VMEM((devices * 8, LANES), F32),
        ],
        compiler_params=pltpu.CompilerParams(dimension_semantics=("arbitrary",)),
        name="pack_loads",
    )(moment, weights, blk, own, node)


def position(grid):
    return lax.axis_index("gx"), lax.axis_index("gy")


def greet_all(grid):
    ix, iy = position(grid)
    devices = grid[0] * grid[1]
    me = ix * grid[1] + iy
    barrier = pltpu.get_barrier_semaphore()

    def signal(j, carry):
        other = lax.rem(me + j, devices)
        pl.semaphore_signal(
            barrier, inc=1, device_id=(lax.div(other, grid[1]), lax.rem(other, grid[1])),
            device_id_type=MESH,
        )
        return carry

    lax.fori_loop(1, devices, signal, 0)
    pl.semaphore_wait(barrier, devices - 1)


def broadcast_copy(grid, j, source, target, send_sem, recv_sem):
    ix, iy = position(grid)
    devices = grid[0] * grid[1]
    me = ix * grid[1] + iy
    other = lax.rem(me + j, devices)
    return pltpu.make_async_remote_copy(
        src_ref=source(other),
        dst_ref=target(me),
        send_sem=send_sem.at[j],
        recv_sem=recv_sem.at[j],
        device_id=(lax.div(other, grid[1]), lax.rem(other, grid[1])),
        device_id_type=MESH,
    )


def to_all(grid, source, target, send_sem, recv_sem, start):
    def body(j, carry):
        copy = broadcast_copy(grid, j, source, target, send_sem, recv_sem)
        if start:
            copy.start()
        else:
            copy.wait()
        return carry

    lax.fori_loop(1, grid[0] * grid[1], body, 0)


def neighbour_copy(grid, dx, dy, source, target, send_sem, recv_sem):
    ix, iy = position(grid)
    return pltpu.make_async_remote_copy(
        src_ref=source,
        dst_ref=target,
        send_sem=send_sem,
        recv_sem=recv_sem,
        device_id=(lax.rem(ix + dx + grid[0], grid[0]), lax.rem(iy + dy + grid[1], grid[1])),
        device_id_type=MESH,
    )


def rim_copies(grid, field, side, strip, send_sem, recv_sem):
    rows = field.shape[1]
    copies = [
        neighbour_copy(grid, 0, 1, field, side.at[0], send_sem.at[0], recv_sem.at[0]),
        neighbour_copy(grid, 0, -1, field, side.at[1], send_sem.at[1], recv_sem.at[1]),
    ]
    for k in range(3):
        dy = 1 - k
        copies.append(
            neighbour_copy(
                grid, 1, dy, field.at[:, pl.ds(rows - 8, 8), :], strip.at[k],
                send_sem.at[2 + k], recv_sem.at[2 + k],
            )
        )
    for k in range(3):
        dy = 1 - k
        copies.append(
            neighbour_copy(
                grid, -1, dy, field.at[:, pl.ds(0, 8), :], strip.at[3 + k],
                send_sem.at[5 + k], recv_sem.at[5 + k],
            )
        )
    return copies


def lines_of(ref, sources, row, parts):
    return jnp.concatenate(
        [ref[source, row + p : row + p + 1] for source in sources for p in range(parts)], axis=1
    )


def sources_of(grid, step, count):
    ix, iy = position(grid)
    devices = grid[0] * grid[1]
    me = ix * grid[1] + iy
    return [lax.rem(me + devices - lax.rem(step * count + d + 1, devices), devices) for d in range(count)]


def node_hots(ref, sources, parts, rows, cols):
    node = lines_of(ref, sources, 3 * parts, parts).astype(jnp.int32)
    half = rows // 2 * cols
    top = node // half
    rest = node - top * half
    row = rest // cols
    col = rest - row * cols + top * cols
    width = len(sources) * parts * LANES
    row_hot = iota((rows // 2, width), 0) == row
    col_hot = (iota((2 * cols, width), 0) == col).astype(F32).astype(BF16)
    return row_hot, col_hot


def gather_force(grid, parts, pay, force, arrived):
    devices = pay.shape[0]
    rows, cols = force.shape[1:]
    half = rows // 2
    count = math.gcd(devices, 4)

    def one(step, total):
        sources = sources_of(grid, step, count)
        for d in range(count):
            arrived(step * count + d + 1)
        row_hot, col_hot = node_hots(pay, sources, parts, rows, cols)
        highs = []
        lows = []
        for c in range(3):
            value = lines_of(pay, sources, c * parts, parts)
            high = value.astype(BF16).astype(F32)
            highs.append(jnp.where(row_hot, high, 0.0).astype(BF16))
            lows.append(jnp.where(row_hot, value - high, 0.0).astype(BF16))
        return total + dot_nt(jnp.concatenate(highs + lows, axis=0), col_hot)

    total = lax.fori_loop(0, devices // count, one, jnp.zeros((6 * half, 2 * cols), F32))
    total = total[: 3 * half] + total[3 * half :]
    for c in range(3):
        piece = total[c * half : (c + 1) * half]
        force[c] = jnp.concatenate([piece[:, :cols], piece[:, cols:]], axis=0)


def pick_nodes(grid, parts, field, pay, out, ready):
    devices = pay.shape[0]
    rows, cols = field[0].shape
    half = rows // 2
    count = math.gcd(devices, 4)
    wide = [jnp.concatenate([f[:half], f[half:]], axis=1) for f in field]
    high, low = halves(jnp.concatenate(wide, axis=0))
    left = jnp.concatenate([high, low], axis=0)

    def one(step, carry):
        sources = sources_of(grid, step, count)
        row_hot, col_hot = node_hots(pay, sources, parts, rows, cols)
        found = dot_nn(left, col_hot)
        found = found[: 3 * half] + found[3 * half :]
        values = [
            jnp.sum(
                jnp.where(row_hot, found[c * half : (c + 1) * half], 0.0), axis=0, keepdims=True
            )
            for c in range(3)
        ]
        for d in range(count):
            pieces = []
            for value in values:
                for p in range(parts):
                    at = (d * parts + p) * LANES
                    pieces.append(value[:, at : at + LANES])
            pieces.append(jnp.zeros((8 - 3 * parts, LANES), F32))
            out[sources[d]] = jnp.concatenate(pieces, axis=0)
        for d in range(count):
            ready(step * count + d + 1)
        return carry

    lax.fori_loop(0, devices // count, one, 0)


def with_rim(centre, side, strip, c):
    rows, cols = centre.shape[1:]
    left_half = iota((rows, cols), 1) < cols // 2
    main = jnp.concatenate([centre[c], jnp.where(left_half, side[1, c], side[0, c])], axis=1)
    low = iota((8, cols), 0) < 4
    left_strip = iota((8, cols), 1) < cols // 2
    below = jnp.where(low, strip[4, c], strip[1, c])
    corner = jnp.where(
        low,
        jnp.where(left_strip, strip[5, c], strip[3, c]),
        jnp.where(left_strip, strip[2, c], strip[0, c]),
    )
    return jnp.concatenate([main, jnp.concatenate([below, corner], axis=1)], axis=0)


def couple_kernel(
    grid, parts, stiff, pay, xu, xd, yu, yd, modulus_ref, live_ref, mass_ref,
    force_out, image_out, scal_out, back_f_in, back_q_in, xu_in, xd_in, yu_in, yd_in, corner_in,
    pay_in, back_f, back_q, stat, stat_side, stat_strip, force, side, strip, sums,
    pay_send, pay_recv, backf_send, backf_recv, backq_send, backq_recv, lb_send, lb_recv,
    stat_send, stat_recv, rim_send, rim_recv, sum_send, sum_recv,
):
    ix, iy = position(grid)
    devices = grid[0] * grid[1]
    me = ix * grid[1] + iy
    rows, cols = force.shape[1:]
    full = (rows + 8, 2 * cols)
    stat[0] = modulus_ref[...]
    stat[1] = live_ref[...].astype(F32)
    stat[2] = mass_ref[...]
    greet_all(grid)
    to_all(grid, lambda o: pay.at[o], lambda m: pay_in.at[m], pay_send, pay_recv, True)
    stat_copies = rim_copies(grid, stat, stat_side, stat_strip, stat_send, stat_recv)
    nx = yu.shape[1]
    plan = [
        (1, 0, xu, xu_in),
        (-1, 0, xd, xd_in),
        (0, 1, yu, yu_in),
        (0, -1, yd, yd_in),
    ]
    for k, q in enumerate(diagonal):
        dx, dy, _ = lattice_dirs[q]
        edge = yu.at[y_up.index(q)] if dy == 1 else yd.at[y_down.index(q)]
        plan.append((dx, dy, edge.at[nx - 1 if dx == 1 else 0], corner_in.at[k]))
    lb_copies = [
        neighbour_copy(grid, dx, dy, source, target, lb_send.at[number], lb_recv.at[number])
        for number, (dx, dy, source, target) in enumerate(plan)
    ]
    pay_in[me] = pay[me]
    for copy in stat_copies + lb_copies:
        copy.start()

    def pay_arrived(j):
        @pl.when(j < devices)
        def _():
            broadcast_copy(
                grid, j, lambda o: pay.at[o], lambda m: pay_in.at[m], pay_send, pay_recv
            ).wait()

    gather_force(grid, parts, pay_in, force, pay_arrived)
    copies = rim_copies(grid, force, side, strip, rim_send, rim_recv)
    for copy in copies:
        copy.start()

    def back_copy(j, back, back_in, send_sem, recv_sem):
        other = lax.rem(me + devices - j, devices)
        return pltpu.make_async_remote_copy(
            src_ref=back.at[other],
            dst_ref=back_in.at[me],
            send_sem=send_sem.at[j],
            recv_sem=recv_sem.at[j],
            device_id=(lax.div(other, grid[1]), lax.rem(other, grid[1])),
            device_id_type=MESH,
        )

    def sender(*args):
        def ready(j):
            @pl.when(j < devices)
            def _():
                back_copy(j, *args).start()

        return ready

    def wait_back(*args):
        def body(j, carry):
            back_copy(j, *args).wait()
            return carry

        lax.fori_loop(1, devices, body, 0)

    f_args = (back_f, back_f_in, backf_send, backf_recv)
    q_args = (back_q, back_q_in, backq_send, backq_recv)
    own = [force[c] for c in range(3)]
    for c in range(3):
        force_out[c] = own[c]
    pick_nodes(grid, parts, own, pay_in, back_f, sender(*f_args))
    back_f_in[me] = back_f[me]

    def back_row(a):
        return pltpu.roll(a, full[0] - 1, 0)

    def back_col(a):
        return pltpu.roll(a, full[1] - 1, 1)

    for copy in stat_copies:
        copy.wait()
    moduli = with_rim(stat, stat_side, stat_strip, 0)
    live = with_rim(stat, stat_side, stat_strip, 1)
    mass = with_rim(stat, stat_side, stat_strip, 2)
    next_row = back_row(moduli)
    scale = live * (moduli + next_row + back_col(moduli) + back_col(next_row)) * 0.25

    def operate(fields):
        down = [back_row(f) for f in fields]
        corners = (
            list(fields) + down + [back_col(f) for f in fields] + [back_col(f) for f in down]
        )
        results = []
        for k in range(12):
            total = stiff[k, 0] * corners[0]
            for l in range(1, 12):
                total = total + stiff[k, l] * corners[l]
            results.append(scale * total)
        images = []
        for c in range(3):
            right = results[6 + c] + pltpu.roll(results[9 + c], 1, 0)
            images.append(
                mass * fields[c]
                + results[c]
                + pltpu.roll(results[3 + c], 1, 0)
                + pltpu.roll(right, 1, 1)
            )
        return images

    def inner(a, b):
        total = a[0] * b[0]
        for c in range(1, 3):
            total = total + a[c] * b[c]
        return jnp.sum(jnp.sum(total, axis=0, keepdims=True), axis=1, keepdims=True)

    for copy in copies:
        copy.wait()
    field = [with_rim(force, side, strip, c) for c in range(3)]
    image = operate(field)
    second = operate(image)
    f = [a[:rows, :cols] for a in field]
    q = [a[:rows, :cols] for a in image]
    s = [a[:rows, :cols] for a in second]
    for c in range(3):
        image_out[c] = q[c]
    ff, fq, qq, qs = inner(f, f), inner(f, q), inner(q, q), inner(q, s)
    guess = jnp.where(qq > 0.0, fq / jnp.where(qq > 0.0, qq, 1.0), 0.0)
    r0 = [f[c] - guess * q[c] for c in range(3)]
    u0 = [q[c] - guess * s[c] for c in range(3)]
    mine = [ff, fq, qq, qs, guess, inner(r0, r0), inner(r0, q), inner(r0, u0), inner(r0, s), inner(q, u0)]
    lane = iota((1, LANES), 1)
    line = jnp.zeros((1, LANES), F32)
    for k, value in enumerate(mine):
        line = jnp.where(lane == k, value, line)
    sums[me] = line
    to_all(grid, lambda o: sums.at[me], lambda m: sums.at[m], sum_send, sum_recv, True)
    pick_nodes(grid, parts, q, pay_in, back_q, sender(*q_args))
    back_q_in[me] = back_q[me]
    to_all(grid, lambda o: sums.at[me], lambda m: sums.at[m], sum_send, sum_recv, False)
    every = sums[...].reshape(devices, LANES)
    ff, fq, qq, qs, guess, r0r0, r0q, r0u0, r0s, qu0 = [every[:, k : k + 1] for k in range(len(mine))]

    def total(value):
        return jnp.sum(value, axis=0, keepdims=True)

    ff_all, fq_all = total(ff), total(fq)
    first = ff_all / fq_all
    off = guess - first
    rr = total(r0r0 + off * (2.0 * r0q + off * qq))
    rs = total(r0u0 + off * (r0s + qu0 + off * qs))
    rq = total(r0q + off * qq)
    ratio = rr / ff_all
    step_two = rr / (rs + 2.0 * ratio * rq + ratio * ratio * fq_all)
    alpha = first + step_two * (1.0 + ratio)
    beta = -(step_two * first)
    scal_out[...] = jnp.where(lane == 0, alpha, jnp.where(lane == 1, beta, 0.0))
    wait_back(*f_args)
    wait_back(*q_args)
    for copy in lb_copies:
        copy.wait()


def couple(grid, parts, stiff, pay, xu, xd, yu, yd, modulus, live, mass):
    devices = grid[0] * grid[1]
    depth = xu.shape[2]
    patch = (3,) + mass.shape
    shapes = [
        patch, patch, (1, LANES), pay.shape, pay.shape, xu.shape, xd.shape, yu.shape, yd.shape,
        (4, 1, depth),
    ]
    vmem = pl.BlockSpec(memory_space=pltpu.VMEM)
    rim = [pltpu.VMEM((2,) + patch, F32), pltpu.VMEM((6, 3, 8, patch[2]), F32)]
    to_each = pltpu.SemaphoreType.DMA((devices,))
    to_near = pltpu.SemaphoreType.DMA((8,))
    return pl.pallas_call(
        functools.partial(couple_kernel, grid, parts),
        in_specs=[pl.BlockSpec(memory_space=pltpu.SMEM)] + [vmem] * 8,
        out_specs=[vmem] * len(shapes),
        out_shape=[jax.ShapeDtypeStruct(shape, F32) for shape in shapes],
        scratch_shapes=[
            pltpu.VMEM(pay.shape, F32),
            pltpu.VMEM(pay.shape, F32),
            pltpu.VMEM(pay.shape, F32),
            pltpu.VMEM(patch, F32),
            *rim,
            pltpu.VMEM(patch, F32),
            *rim,
            pltpu.VMEM((devices, 1, LANES), F32),
            to_each, to_each, to_each, to_each, to_each, to_each, to_near, to_near,
            to_near, to_near, to_near, to_near, to_each, to_each,
        ],
        compiler_params=pltpu.CompilerParams(collective_id=0, has_side_effects=True),
        name="couple",
    )(stiff, pay, xu, xd, yu, yd, modulus, live, mass)


def forcing_kernel(
    parts, scal, force_ref, image_ref, backf_ref, backq_ref, w_ref, blk_ref, own_ref, slot_ref,
    out_ref, disp_ref, back_cat,
):
    step = pl.program_id(0)
    devices = backf_ref.shape[0]
    blocks = out_ref.shape[0] // 3
    chunk = w_ref.shape[0]

    @pl.when(step == 0)
    def _():
        alpha = scal[0, 0]
        beta = scal[0, 1]
        disp_ref[...] = alpha * force_ref[...] + beta * image_ref[...]
        back = alpha * backf_ref[...] + beta * backq_ref[...]
        high, low = halves(back.reshape(devices * 8, LANES))
        back_cat[...] = jnp.concatenate([high, low], axis=1)
        out_ref[...] = jnp.zeros_like(out_ref)

    slot_id = slot_ref[...]
    part = slot_id // LANES
    place = slot_id - part * LANES
    slot_hot = (iota((LANES, chunk), 0) == place).astype(F32).astype(BF16)
    found = dot_nn(back_cat[...], jnp.concatenate([slot_hot, slot_hot], axis=0))
    mine = (iota((devices * 8, chunk), 0) // 8) == own_ref[...]
    lines = jnp.sum(jnp.where(mine, found, 0.0).reshape(devices, 8, chunk), axis=0)
    channel = iota((8, chunk), 0) // parts
    in_part = (iota((8, chunk), 0) - channel * parts) == part
    here = iota((blocks, chunk), 0) == blk_ref[...]
    highs = []
    lows = []
    for c in range(3):
        moved = coupling * jnp.sum(
            jnp.where(in_part & (channel == c), lines, 0.0), axis=0, keepdims=True
        )
        high = moved.astype(BF16).astype(F32)
        highs.append(jnp.where(here, high, 0.0).astype(BF16))
        lows.append(jnp.where(here, moved - high, 0.0).astype(BF16))
    high = jnp.concatenate(highs, axis=0)
    low = jnp.concatenate(lows, axis=0)
    w_high, w_low = halves(w_ref[...])
    out_ref[...] += dot_nn(
        jnp.concatenate([high, low, high], axis=1),
        jnp.concatenate([w_high, w_high, w_low], axis=0),
    )


def forcing_of(parts, blocks, scal, force, image, back_f, back_q, weights, blk, own, slot):
    records, depth = weights.shape
    chunk = 1024
    row_spec = pl.BlockSpec((1, chunk), lambda i: (0, i))
    whole3 = lambda i: (0, 0, 0)
    return pl.pallas_call(
        functools.partial(forcing_kernel, parts),
        grid=(records // chunk,),
        in_specs=[
            pl.BlockSpec(memory_space=pltpu.SMEM),
            pl.BlockSpec(force.shape, whole3),
            pl.BlockSpec(force.shape, whole3),
            pl.BlockSpec(back_f.shape, whole3),
            pl.BlockSpec(back_f.shape, whole3),
            pl.BlockSpec((chunk, depth), lambda i: (i, 0)),
            row_spec,
            row_spec,
            row_spec,
        ],
        out_specs=[
            pl.BlockSpec((3 * blocks, depth), lambda i: (0, 0)),
            pl.BlockSpec(force.shape, whole3),
        ],
        out_shape=[
            jax.ShapeDtypeStruct((3 * blocks, depth), F32),
            jax.ShapeDtypeStruct(force.shape, F32),
        ],
        scratch_shapes=[pltpu.VMEM((back_f.shape[0] * 8, 2 * LANES), BF16)],
        compiler_params=pltpu.CompilerParams(dimension_semantics=("arbitrary",)),
        name="forcing",
    )(scal, force, image, back_f, back_q, weights, blk, own, slot)


def stream_kernel(
    cur, prev_ref, next_ref, forcing, xu, xd, yu, yd, yu_prev, yu_next, yd_prev, yd_next, corner,
    out_ref,
):
    step = pl.program_id(0)
    last = pl.num_programs(0) - 1
    rows, ny, nz = cur.shape[1:]
    fields = [forcing[c] for c in range(3)]

    def shifted(block, before, after, dx):
        if dx == 1:
            return jnp.concatenate([before[None], block[: rows - 1]], axis=0)
        if dx == -1:
            return jnp.concatenate([block[1:], after[None]], axis=0)
        return block

    for q in range(19):
        dx, dy, dz = lattice_dirs[q]
        before = after = None
        if dx == 1:
            before = jnp.where(step == 0, xu[x_up.index(q)], prev_ref[q, 0])
        if dx == -1:
            after = jnp.where(step == last, xd[x_down.index(q)], next_ref[q, 0])
        moved = shifted(cur[q], before, after, dx)
        if dy != 0:
            k = y_up.index(q) if dy == 1 else y_down.index(q)
            edge = (yu if dy == 1 else yd)[k]
            if dx == 1:
                before = (yu_prev if dy == 1 else yd_prev)[k, 0]
                before = jnp.where(step == 0, corner[diagonal.index(q)], before)
            if dx == -1:
                after = (yu_next if dy == 1 else yd_next)[k, 0]
                after = jnp.where(step == last, corner[diagonal.index(q)], after)
            edge = shifted(edge, before, after, dx)
            turned = pltpu.roll(moved, dy % ny, 1)
            at_edge = iota((rows, ny, nz), 1) == (0 if dy == 1 else ny - 1)
            moved = jnp.where(at_edge, jnp.broadcast_to(edge, (rows, ny, nz)), turned)
        if dz != 0:
            moved = pltpu.roll(moved, dz % nz, 2)
        projected = combine_dirs(fields, lattice_dirs[q])
        if projected is not None:
            moved = moved + (3.0 * lattice_weights[q]) * projected
        out_ref[q] = moved


def stream(relaxed, forcing, xu, xd, yu, yd, corner):
    _, nx, ny, nz = relaxed.shape
    rows = 8
    steps = nx // rows
    before = lambda i: (0, (i * rows + nx - 1) % nx, 0, 0)
    after = lambda i: (0, (i * rows + rows) % nx, 0, 0)
    whole3 = lambda i: (0, 0, 0)
    blocked = lambda i: (0, i, 0, 0)
    return pl.pallas_call(
        stream_kernel,
        grid=(steps,),
        in_specs=[
            pl.BlockSpec((19, rows, ny, nz), blocked),
            pl.BlockSpec((19, 1, ny, nz), before),
            pl.BlockSpec((19, 1, ny, nz), after),
            pl.BlockSpec((3, rows, ny, nz), blocked),
            pl.BlockSpec((5, ny, nz), whole3),
            pl.BlockSpec((5, ny, nz), whole3),
            pl.BlockSpec((5, rows, 1, nz), blocked),
            pl.BlockSpec((5, rows, 1, nz), blocked),
            pl.BlockSpec((5, 1, 1, nz), before),
            pl.BlockSpec((5, 1, 1, nz), after),
            pl.BlockSpec((5, 1, 1, nz), before),
            pl.BlockSpec((5, 1, 1, nz), after),
            pl.BlockSpec((4, 1, nz), whole3),
        ],
        out_specs=pl.BlockSpec((19, rows, ny, nz), blocked),
        out_shape=jax.ShapeDtypeStruct((19, nx, ny, nz), F32),
        compiler_params=pltpu.CompilerParams(dimension_semantics=("arbitrary",)),
        name="stream",
    )(relaxed, relaxed, relaxed, forcing, xu, xd, yu, yd, yu, yu, yd, yd, corner)


def per_device(
    grid, populations, mass, modulus, cell_live, stiff_ref, rec_block, rec_owner, rec_node,
    rbf_weight,
):
    devices = grid[0] * grid[1]
    _, nx, ny, nz = populations.shape
    records = rec_block.shape[0]
    rows, cols = mass.shape
    capacity = 2 * records // devices
    parts = -(-capacity // LANES)
    relaxed, moment, xu, xd, yu, yd = collide(populations)
    blk = rec_block.reshape(1, records)
    own = rec_owner.reshape(1, records)
    node = rec_node.reshape(1, records)
    pay, slot = pack_loads(
        devices, parts, cols, moment.reshape(3 * nx * ny, nz), rbf_weight, blk, own, node
    )
    force, image, scal, back_f, back_q, xu, xd, yu, yd, corner = couple(
        grid, parts, stiff_ref, pay, xu, xd, yu, yd, modulus, cell_live, mass
    )
    forcing, displacement = forcing_of(
        parts, nx * ny, scal, force, image, back_f, back_q, rbf_weight, blk, own, slot
    )
    out = stream(relaxed, forcing.reshape(3, nx, ny, nz), xu, xd, yu, yd, corner)
    return out, displacement


def solution(mesh):
    grid = (mesh.shape["gx"], mesh.shape["gy"])
    in_specs = (
        P(None, "gx", "gy", None),
        P("gx", "gy"),
        P("gx", "gy"),
        P("gx", "gy"),
        P(),
        P(("gx", "gy")),
        P(("gx", "gy"), None),
        P(("gx", "gy")),
        P(("gx", "gy"), None),
    )
    out_specs = (P(None, "gx", "gy", None), P(None, "gx", "gy"))
    return jax.shard_map(
        functools.partial(per_device, grid), mesh=mesh, in_specs=in_specs, out_specs=out_specs,
        check_vma=False,
    )
```

```python
import functools
import math

import jax
import jax.numpy as jnp
from jax import lax
from jax.experimental import pallas as pl
from jax.experimental.pallas import tpu as pltpu
from jax.sharding import PartitionSpec as P

MESH = pl.DeviceIdType.MESH
F32 = jnp.float32
BF16 = jnp.bfloat16
LANES = 128

lattice_dirs = (
    (0, 0, 0),
    (1, 0, 0),
    (-1, 0, 0),
    (0, 1, 0),
    (0, -1, 0),
    (0, 0, 1),
    (0, 0, -1),
    (1, 1, 0),
    (-1, -1, 0),
    (1, -1, 0),
    (-1, 1, 0),
    (1, 0, 1),
    (-1, 0, -1),
    (1, 0, -1),
    (-1, 0, 1),
    (0, 1, 1),
    (0, -1, -1),
    (0, 1, -1),
    (0, -1, 1),
)
lattice_weights = (1.0 / 3.0,) + (1.0 / 18.0,) * 6 + (1.0 / 36.0,) * 12
relax_rate = 1.25
coupling = 0.1

x_up = [q for q in range(19) if lattice_dirs[q][0] == 1]
x_down = [q for q in range(19) if lattice_dirs[q][0] == -1]
y_up = [q for q in range(19) if lattice_dirs[q][1] == 1]
y_down = [q for q in range(19) if lattice_dirs[q][1] == -1]
diagonal = [q for q in range(19) if lattice_dirs[q][0] != 0 and lattice_dirs[q][1] != 0]


def combine_dirs(fields, direction):
    total = None
    for axis_pos in range(3):
        if direction[axis_pos] != 0:
            field = fields[axis_pos]
            if total is None:
                total = field if direction[axis_pos] == 1 else -field
            else:
                total = total + field if direction[axis_pos] == 1 else total - field
    return total


def halves(values):
    high = values.astype(BF16)
    low = (values - high.astype(F32)).astype(BF16)
    return high, low


def iota(shape, dim):
    return lax.broadcasted_iota(jnp.int32, shape, dim)


def dot_nt(left, right):
    return lax.dot_general(left, right, (((1,), (1,)), ((), ())), preferred_element_type=F32)


def dot_nn(left, right):
    return lax.dot_general(left, right, (((1,), (0,)), ((), ())), preferred_element_type=F32)


def position(grid):
    return lax.axis_index("gx"), lax.axis_index("gy")


def greet_all(grid):
    ix, iy = position(grid)
    devices = grid[0] * grid[1]
    me = ix * grid[1] + iy
    barrier = pltpu.get_barrier_semaphore()

    def signal(j, carry):
        other = lax.rem(me + j, devices)
        pl.semaphore_signal(
            barrier, inc=1, device_id=(lax.div(other, grid[1]), lax.rem(other, grid[1])),
            device_id_type=MESH,
        )
        return carry

    lax.fori_loop(1, devices, signal, 0)


def await_all(grid):
    pl.semaphore_wait(pltpu.get_barrier_semaphore(), grid[0] * grid[1] - 1)


def broadcast_copy(grid, j, source, target, send_sem, recv_sem):
    ix, iy = position(grid)
    devices = grid[0] * grid[1]
    me = ix * grid[1] + iy
    other = lax.rem(me + j, devices)
    return pltpu.make_async_remote_copy(
        src_ref=source(other),
        dst_ref=target(me),
        send_sem=send_sem.at[j],
        recv_sem=recv_sem.at[j],
        device_id=(lax.div(other, grid[1]), lax.rem(other, grid[1])),
        device_id_type=MESH,
    )


def to_all(grid, source, target, send_sem, recv_sem, start):
    def body(j, carry):
        copy = broadcast_copy(grid, j, source, target, send_sem, recv_sem)
        if start:
            copy.start()
        else:
            copy.wait()
        return carry

    lax.fori_loop(1, grid[0] * grid[1], body, 0)


def neighbour_copy(grid, dx, dy, source, target, send_sem, recv_sem):
    ix, iy = position(grid)
    return pltpu.make_async_remote_copy(
        src_ref=source,
        dst_ref=target,
        send_sem=send_sem,
        recv_sem=recv_sem,
        device_id=(lax.rem(ix + dx + grid[0], grid[0]), lax.rem(iy + dy + grid[1], grid[1])),
        device_id_type=MESH,
    )


def pack_side(field, side_out):
    rows, cols = field.shape[1:]
    for c in range(3):
        tall = jnp.concatenate([field[c], jnp.zeros((cols - rows, cols), F32)], axis=0).T
        side_out[0, c] = tall[cols - 8 :]
        side_out[1, c] = tall[:8]


def rim_copies(grid, field, side_out, side, strip, send_sem, recv_sem):
    rows = field.shape[1]
    copies = []
    for k in range(3):
        dy = 1 - k
        copies.append(
            neighbour_copy(
                grid, 1, dy, field.at[:, pl.ds(rows - 8, 8), :], strip.at[k],
                send_sem.at[2 + k], recv_sem.at[2 + k],
            )
        )
        copies.append(
            neighbour_copy(
                grid, -1, dy, field.at[:, pl.ds(0, 8), :], strip.at[3 + k],
                send_sem.at[5 + k], recv_sem.at[5 + k],
            )
        )
    copies.append(
        neighbour_copy(grid, 0, 1, side_out.at[0], side.at[0], send_sem.at[0], recv_sem.at[0])
    )
    copies.append(
        neighbour_copy(grid, 0, -1, side_out.at[1], side.at[1], send_sem.at[1], recv_sem.at[1])
    )
    return copies


def with_rim(centre, side, strip, c):
    rows, cols = centre.shape[1:]
    beside = jnp.concatenate([side[1, c], jnp.zeros((cols - 16, cols), F32), side[0, c]], axis=0)
    main = jnp.concatenate([centre[c], beside.T[:rows]], axis=1)
    low = iota((8, cols), 0) < 4
    left_strip = iota((8, cols), 1) < cols // 2
    below = jnp.where(low, strip[4, c], strip[1, c])
    corner = jnp.where(
        low,
        jnp.where(left_strip, strip[5, c], strip[3, c]),
        jnp.where(left_strip, strip[2, c], strip[0, c]),
    )
    return jnp.concatenate([main, jnp.concatenate([below, corner], axis=1)], axis=0)


def find_slots(devices, node_cols, own_ref, node_ref, slot_ref, slot_hot, node_pay):
    records = own_ref.shape[1]
    slots = slot_hot.shape[0]
    span = 2 * LANES
    steps = records // span
    before = (iota((span, span), 0) <= iota((span, span), 1)).astype(F32).astype(BF16)
    hits = [
        iota((devices, span), 0) == own_ref[:, i * span : (i + 1) * span] for i in range(steps)
    ]
    base = jnp.full((devices, span), -1.0, F32)
    routed = None
    for i in range(steps):
        counts = dot_nn(hits[i].astype(F32).astype(BF16), before)
        slot = jnp.sum(jnp.where(hits[i], counts + base, 0.0), axis=0, keepdims=True)
        base = base + jnp.broadcast_to(counts[:, span - 1 :], (devices, span))
        slot = slot.astype(jnp.int32)
        slot_ref[:, i * span : (i + 1) * span] = slot
        hot = (iota((slots, span), 0) == slot).astype(F32).astype(BF16)
        slot_hot[:, i * span : (i + 1) * span] = hot
        node = node_ref[:, i * span : (i + 1) * span]
        row = node // node_cols
        col = (node - row * node_cols).astype(F32)
        left = jnp.concatenate(
            [jnp.where(hits[i], row.astype(F32), 0.0), jnp.where(hits[i], col, 0.0)], axis=0
        )
        part = dot_nt(left.astype(BF16), hot)
        routed = part if routed is None else routed + part
    nodes = routed[:devices] * float(node_cols) + routed[devices:]
    for o in range(devices):
        node_pay[o] = nodes[o : o + 1]


def moments(pop, mom, row):
    for axis_pos in range(3):
        total = None
        for q in range(19):
            sign = lattice_dirs[q][axis_pos]
            if sign == 1:
                total = pop[q, row] if total is None else total + pop[q, row]
            elif sign == -1:
                total = -pop[q, row] if total is None else total - pop[q, row]
        mom[axis_pos, row] = total


def collide_row(pop, mom, read, yu, yd, row):
    rows, cols, depth = read.shape[1:]
    pops = [pop[q, row] for q in range(19)]
    density = pops[0]
    for q in range(1, 19):
        density = density + pops[q]
    inverse = 1.0 / density
    velocity = [mom[axis_pos, row] * inverse for axis_pos in range(3)]
    squared = velocity[0] * velocity[0] + velocity[1] * velocity[1] + velocity[2] * velocity[2]
    rest = 1.0 - 1.5 * squared
    scaled = {w: (relax_rate * w) * density for w in sorted(set(lattice_weights))}
    ups = lax.rem(row + 1, rows)
    downs = lax.rem(row + rows - 1, rows)
    for q in range(19):
        dx, dy, dz = lattice_dirs[q]
        projected = combine_dirs(velocity, lattice_dirs[q])
        bracket = rest
        if projected is not None:
            bracket = rest + projected * (3.0 + 4.5 * projected)
        value = (1.0 - relax_rate) * pops[q] + scaled[lattice_weights[q]] * bracket
        if dz != 0:
            value = pltpu.roll(value, dz % depth, 1)
        if dy != 0:
            value = pltpu.roll(value, dy % cols, 0)
        at = ups if dx == 1 else downs if dx == -1 else row
        read[q, at] = value
        if dy == 1:
            yu[y_up.index(q), at] = value[0:1]
        if dy == -1:
            yd[y_down.index(q), at] = value[cols - 1 : cols]


def mend_edges(read, xu, xd, yu, yd, corner):
    rows, cols, depth = read.shape[1:]
    for k, q in enumerate(x_up):
        read[q, 0] = xu[k]
    for k, q in enumerate(x_down):
        read[q, rows - 1] = xd[k]

    def one(row, carry):
        for k, q in enumerate(y_up):
            read[q, row, 0:1] = yu[k, row]
        for k, q in enumerate(y_down):
            read[q, row, cols - 1 : cols] = yd[k, row]
        return carry

    lax.fori_loop(0, rows, one, 0, unroll=4)
    for k, q in enumerate(diagonal):
        dx, dy, _ = lattice_dirs[q]
        at = 0 if dy == 1 else cols - 1
        read[q, 0 if dx == 1 else rows - 1, at : at + 1] = corner[k]


def sources_of(grid, step, count):
    ix, iy = position(grid)
    devices = grid[0] * grid[1]
    me = ix * grid[1] + iy
    return [
        lax.rem(me + devices - lax.rem(step * count + d + 1, devices), devices)
        for d in range(count)
    ]


def node_parts(node, rows, cols):
    node = node.astype(jnp.int32)
    half = rows // 2 * cols
    top = node // half
    rest = node - top * half
    row = rest // cols
    return row, rest - row * cols + top * cols


def lane_row(ref, source, c, parts):
    return jnp.concatenate(
        [ref[source, p * 3 + c : p * 3 + c + 1] for p in range(parts)], axis=1
    )


def gather_force(grid, parts, node_in, node_hot, pay, force, arrived):
    devices = pay.shape[0]
    rows, cols = force.shape[1:]
    half = rows // 2
    slots = parts * LANES
    count = math.gcd(devices, 4)

    def one(step, total):
        sources = sources_of(grid, step, count)
        for d in range(count):
            arrived(step * count + d + 1)
        for source in sources:
            row, _ = node_parts(node_in[source], rows, cols)
            row_hot = iota((half, slots), 0) == row
            highs = []
            lows = []
            for c in range(3):
                value = lane_row(pay, source, c, parts)
                high = value.astype(BF16).astype(F32)
                highs.append(jnp.where(row_hot, high, 0.0).astype(BF16))
                lows.append(jnp.where(row_hot, value - high, 0.0).astype(BF16))
            total = total + dot_nt(jnp.concatenate(highs + lows, axis=0), node_hot[source])
        return total

    total = lax.fori_loop(0, devices // count, one, jnp.zeros((6 * half, 2 * cols), F32))
    total = total[: 3 * half] + total[3 * half :]
    for c in range(3):
        piece = total[c * half : (c + 1) * half]
        force[c] = jnp.concatenate([piece[:, :cols], piece[:, cols:]], axis=0)


def pick_nodes(grid, parts, field, node_in, node_hot, out, ready):
    devices = out.shape[0]
    rows, cols = field[0].shape
    half = rows // 2
    slots = parts * LANES
    count = math.gcd(devices, 4)
    wide = [jnp.concatenate([f[:half], f[half:]], axis=1) for f in field]
    high, low = halves(jnp.concatenate(wide, axis=0))
    left = jnp.concatenate([high, low], axis=0)

    def one(step, carry):
        sources = sources_of(grid, step, count)
        for source in sources:
            row, _ = node_parts(node_in[source], rows, cols)
            row_hot = iota((half, slots), 0) == row
            found = dot_nn(left, node_hot[source])
            found = found[: 3 * half] + found[3 * half :]
            values = [
                jnp.sum(
                    jnp.where(row_hot, found[c * half : (c + 1) * half], 0.0), axis=0, keepdims=True
                )
                for c in range(3)
            ]
            out[source] = jnp.concatenate(
                [value[:, p * LANES : (p + 1) * LANES] for p in range(parts) for value in values],
                axis=0,
            )
        for d in range(count):
            ready(step * count + d + 1)
        return carry

    lax.fori_loop(0, devices // count, one, 0)


def couple_kernel(
    grid, parts, stiff, pop_hbm, w_hbm, blk_hbm, own_hbm, node_hbm, modulus_ref, live_ref, mass_ref,
    read_out, turned_out, force_out, image_out, scal_out, slot_out, back_f_in, back_q_in,
    pop, mom, mom_cat, w, turned, blk, own, node, slot_hot, read, loads,
    xu_in, xd_in, yu_out, yd_out, yu_in, yd_in, corner_in,
    node_pay, node_in, node_hot, pay, pay_in, back_f, back_q,
    stat, stat_out, stat_side, stat_strip, force, side_out, side, strip, sums,
    pop_sem, w_sem, small_sem, turned_sem, read_sem,
    node_send, node_recv, pay_send, pay_recv, backf_send, backf_recv, backq_send, backq_recv,
    lb_send, lb_recv, stat_send, stat_recv, rim_send, rim_recv, sum_send, sum_recv,
):
    ix, iy = position(grid)
    devices = grid[0] * grid[1]
    me = ix * grid[1] + iy
    rows, cols = force.shape[1:]
    full = (rows + 8, 2 * cols)
    nx, ny, nz = read.shape[1:]
    blocks = nx * ny
    records = w.shape[0]
    slots = parts * LANES
    greet_all(grid)
    small = [
        pltpu.make_async_copy(source, target, small_sem.at[k])
        for k, (source, target) in enumerate([(own_hbm, own), (node_hbm, node), (blk_hbm, blk)])
    ]
    pop_rows = nx // 4
    pop_copies = [
        pltpu.make_async_copy(
            pop_hbm.at[:, pl.ds(k * pop_rows, pop_rows)], pop.at[:, pl.ds(k * pop_rows, pop_rows)],
            pop_sem.at[k],
        )
        for k in range(4)
    ]
    span = 4 * LANES
    steps = records // span

    def w_copy(k):
        at = pl.multiple_of(k * span, span)
        return pltpu.make_async_copy(w_hbm.at[pl.ds(at, span)], w.at[pl.ds(at, span)], w_sem.at[k])

    def turned_copy(k):
        at = pl.multiple_of(k * span, span)
        return pltpu.make_async_copy(
            turned.at[:, pl.ds(at, span)], turned_out.at[:, pl.ds(at, span)], turned_sem.at[k]
        )

    for copy in small + pop_copies:
        copy.start()
    for k in range(steps):
        w_copy(k).start()
    stat[0] = modulus_ref[...]
    stat[1] = live_ref[...].astype(F32)
    stat[2] = mass_ref[...]
    pack_side(stat, stat_out)
    for copy in small:
        copy.wait()
    find_slots(devices, cols, own, node, slot_out, slot_hot, node_pay)
    await_all(grid)
    to_all(
        grid, lambda o: node_pay.at[o], lambda m: node_in.at[m], node_send, node_recv, True
    )
    stat_copies = rim_copies(grid, stat, stat_out, stat_side, stat_strip, stat_send, stat_recv)
    for copy in stat_copies:
        copy.start()
    node_in[me] = node_pay[me]

    for k, copy in enumerate(pop_copies):
        copy.wait()

        def moment_row(row, carry):
            moments(pop, mom, row)
            return carry

        lax.fori_loop(k * pop_rows, (k + 1) * pop_rows, moment_row, 0, unroll=2)
    for c in range(3):
        high, low = halves(mom[c].reshape(blocks, nz).T)
        mom_cat[c * nz : (c + 1) * nz, :blocks] = high
        mom_cat[c * nz : (c + 1) * nz, blocks:] = low

    def load_step(k, carry):
        w_copy(k).wait()
        at = pl.multiple_of(k * span, span)
        hot = (iota((blocks, span), 0) == blk[:, pl.ds(at, span)]).astype(F32).astype(BF16)
        picked = dot_nn(mom_cat[...], jnp.concatenate([hot, hot], axis=0))
        flipped = w[pl.ds(at, span), :].T
        turned[:, pl.ds(at, span)] = flipped
        turned_copy(k).start()
        highs = []
        lows = []
        for c in range(3):
            load = jnp.sum(picked[c * nz : (c + 1) * nz] * flipped, axis=0, keepdims=True)
            high = load.astype(BF16).astype(F32)
            highs.append(high)
            lows.append(load - high)
        loads[:, pl.ds(at, span)] = jnp.concatenate(
            highs + lows + [jnp.zeros((2, span), F32)], axis=0
        )
        return carry

    lax.fori_loop(0, steps, load_step, 0)
    routed = None
    for k in range(steps):
        at = k * span
        owners = own[:, at : at + span]
        value = loads[:, at : at + span]
        spread = jnp.concatenate(
            [jnp.where(owners == o, value, 0.0) for o in range(devices)], axis=0
        ).astype(BF16)
        part = dot_nt(spread, slot_hot[:, at : at + span])
        routed = part if routed is None else routed + part
    for o in range(devices):
        tile = routed[o * 8 : o * 8 + 3] + routed[o * 8 + 3 : o * 8 + 6]
        pay[o] = jnp.concatenate(
            [tile[:, p * LANES : (p + 1) * LANES] for p in range(parts)], axis=0
        )
    to_all(grid, lambda o: pay.at[o], lambda m: pay_in.at[m], pay_send, pay_recv, True)
    pay_in[me] = pay[me]

    def collide_step(row, carry):
        collide_row(pop, mom, read, yu_out, yd_out, row)
        return carry

    lax.fori_loop(0, nx, collide_step, 0)
    plan = []
    for k, q in enumerate(x_up):
        plan.append((1, 0, read.at[q, 0], xu_in.at[k]))
    for k, q in enumerate(x_down):
        plan.append((-1, 0, read.at[q, nx - 1], xd_in.at[k]))
    for k, q in enumerate(diagonal):
        dx, dy, _ = lattice_dirs[q]
        edge = yu_out.at[y_up.index(q)] if dy == 1 else yd_out.at[y_down.index(q)]
        plan.append((dx, dy, edge.at[0 if dx == 1 else nx - 1], corner_in.at[k]))
    plan.append((0, 1, yu_out, yu_in))
    plan.append((0, -1, yd_out, yd_in))
    lb_copies = [
        neighbour_copy(grid, dx, dy, source, target, lb_send.at[number], lb_recv.at[number])
        for number, (dx, dy, source, target) in enumerate(plan)
    ]
    to_all(
        grid, lambda o: node_pay.at[o], lambda m: node_in.at[m], node_send, node_recv, False
    )

    def hot_step(d, carry):
        _, col = node_parts(node_in[d], rows, cols)
        node_hot[d] = (iota((2 * cols, slots), 0) == col).astype(F32).astype(BF16)
        return carry

    lax.fori_loop(0, devices, hot_step, 0, unroll=2)

    def pay_arrived(j):
        @pl.when(j < devices)
        def _():
            broadcast_copy(
                grid, j, lambda o: pay.at[o], lambda m: pay_in.at[m], pay_send, pay_recv
            ).wait()

    gather_force(grid, parts, node_in, node_hot, pay_in, force, pay_arrived)
    pack_side(force, side_out)
    copies = rim_copies(grid, force, side_out, side, strip, rim_send, rim_recv)
    for copy in copies + lb_copies:
        copy.start()

    def back_copy(j, back, back_in, send_sem, recv_sem):
        other = lax.rem(me + devices - j, devices)
        return pltpu.make_async_remote_copy(
            src_ref=back.at[other],
            dst_ref=back_in.at[me],
            send_sem=send_sem.at[j],
            recv_sem=recv_sem.at[j],
            device_id=(lax.div(other, grid[1]), lax.rem(other, grid[1])),
            device_id_type=MESH,
        )

    def sender(*args):
        def ready(j):
            @pl.when(j < devices)
            def _():
                back_copy(j, *args).start()

        return ready

    def wait_back(*args):
        def body(j, carry):
            back_copy(j, *args).wait()
            return carry

        lax.fori_loop(1, devices, body, 0)

    f_args = (back_f, back_f_in, backf_send, backf_recv)
    q_args = (back_q, back_q_in, backq_send, backq_recv)
    held = [force[c] for c in range(3)]
    for c in range(3):
        force_out[c] = held[c]
    pick_nodes(grid, parts, held, node_in, node_hot, back_f, sender(*f_args))
    back_f_in[me] = back_f[me]

    def back_row(a):
        return pltpu.roll(a, full[0] - 1, 0)

    def back_col(a):
        return pltpu.roll(a, full[1] - 1, 1)

    for copy in stat_copies:
        copy.wait()
    moduli = with_rim(stat, stat_side, stat_strip, 0)
    live = with_rim(stat, stat_side, stat_strip, 1)
    mass = with_rim(stat, stat_side, stat_strip, 2)
    next_row = back_row(moduli)
    scale = live * (moduli + next_row + back_col(moduli) + back_col(next_row)) * 0.25

    def operate(fields):
        down = [back_row(f) for f in fields]
        corners = (
            list(fields) + down + [back_col(f) for f in fields] + [back_col(f) for f in down]
        )
        results = []
        for k in range(12):
            total = stiff[k, 0] * corners[0]
            for l in range(1, 12):
                total = total + stiff[k, l] * corners[l]
            results.append(scale * total)
        images = []
        for c in range(3):
            right = results[6 + c] + pltpu.roll(results[9 + c], 1, 0)
            images.append(
                mass * fields[c]
                + results[c]
                + pltpu.roll(results[3 + c], 1, 0)
                + pltpu.roll(right, 1, 1)
            )
        return images

    def inner(a, b):
        total = a[0] * b[0]
        for c in range(1, 3):
            total = total + a[c] * b[c]
        return jnp.sum(jnp.sum(total, axis=0, keepdims=True), axis=1, keepdims=True)

    for copy in copies:
        copy.wait()
    field = [with_rim(force, side, strip, c) for c in range(3)]
    image = operate(field)
    second = operate(image)
    f = [a[:rows, :cols] for a in field]
    q = [a[:rows, :cols] for a in image]
    s = [a[:rows, :cols] for a in second]
    for c in range(3):
        image_out[c] = q[c]
    ff, fq, qq, qs = inner(f, f), inner(f, q), inner(q, q), inner(q, s)
    guess = jnp.where(qq > 0.0, fq / jnp.where(qq > 0.0, qq, 1.0), 0.0)
    r0 = [f[c] - guess * q[c] for c in range(3)]
    u0 = [q[c] - guess * s[c] for c in range(3)]
    mine = [
        ff, fq, qq, qs, guess, inner(r0, r0), inner(r0, q), inner(r0, u0), inner(r0, s), inner(q, u0)
    ]
    lane = iota((1, LANES), 1)
    line = jnp.zeros((1, LANES), F32)
    for k, value in enumerate(mine):
        line = jnp.where(lane == k, value, line)
    sums[me] = line
    to_all(grid, lambda o: sums.at[me], lambda m: sums.at[m], sum_send, sum_recv, True)
    pick_nodes(grid, parts, q, node_in, node_hot, back_q, sender(*q_args))
    back_q_in[me] = back_q[me]

    for copy in lb_copies:
        copy.wait()
    mend_edges(read, xu_in, xd_in, yu_in, yd_in, corner_in)
    read_copies = [
        pltpu.make_async_copy(read.at[k], read_out.at[k], read_sem.at[k]) for k in range(19)
    ]
    for copy in read_copies:
        copy.start()
    to_all(grid, lambda o: sums.at[me], lambda m: sums.at[m], sum_send, sum_recv, False)
    every = sums[...].reshape(devices, LANES)
    ff, fq, qq, qs, guess, r0r0, r0q, r0u0, r0s, qu0 = [
        every[:, k : k + 1] for k in range(len(mine))
    ]

    def total(value):
        return jnp.sum(value, axis=0, keepdims=True)

    ff_all, fq_all = total(ff), total(fq)
    first = ff_all / fq_all
    off = guess - first
    rr = total(r0r0 + off * (2.0 * r0q + off * qq))
    rs = total(r0u0 + off * (r0s + qu0 + off * qs))
    rq = total(r0q + off * qq)
    ratio = rr / ff_all
    step_two = rr / (rs + 2.0 * ratio * rq + ratio * ratio * fq_all)
    alpha = first + step_two * (1.0 + ratio)
    beta = -(step_two * first)
    scal_out[...] = jnp.where(lane == 0, alpha, jnp.where(lane == 1, beta, 0.0))

    def turned_wait(k, carry):
        turned_copy(k).wait()
        return carry

    lax.fori_loop(0, steps, turned_wait, 0)
    for copy in read_copies:
        copy.wait()
    wait_back(*f_args)
    wait_back(*q_args)


def couple(grid, parts, stiff, populations, weights, blk, own, node, modulus, live, mass):
    devices = grid[0] * grid[1]
    _, nx, ny, nz = populations.shape
    records = weights.shape[0]
    patch = (3,) + mass.shape
    slots = parts * LANES
    vmem = pl.BlockSpec(memory_space=pltpu.VMEM)
    hbm = pl.BlockSpec(memory_space=pl.ANY)
    rim = [
        pltpu.VMEM((2, 3, 8, patch[2]), F32),
        pltpu.VMEM((2, 3, 8, patch[2]), F32),
        pltpu.VMEM((6, 3, 8, patch[2]), F32),
    ]
    pay = (devices, 3 * parts, LANES)
    back = jax.ShapeDtypeStruct(pay, F32)
    dma = pltpu.SemaphoreType.DMA
    to_each = dma((devices,))
    to_near = dma((8,))
    lines = pltpu.VMEM((1, records), jnp.int32)
    edges = pltpu.VMEM((5, nx, 1, nz), F32)
    return pl.pallas_call(
        functools.partial(couple_kernel, grid, parts),
        in_specs=[pl.BlockSpec(memory_space=pltpu.SMEM)] + [hbm] * 5 + [vmem] * 3,
        out_specs=[hbm, hbm] + [vmem] * 6,
        out_shape=[
            jax.ShapeDtypeStruct(populations.shape, F32),
            jax.ShapeDtypeStruct((nz, records), F32),
            jax.ShapeDtypeStruct(patch, F32),
            jax.ShapeDtypeStruct(patch, F32),
            jax.ShapeDtypeStruct((1, LANES), F32),
            jax.ShapeDtypeStruct((1, records), jnp.int32),
            back,
            back,
        ],
        scratch_shapes=[
            pltpu.VMEM(populations.shape, F32),
            pltpu.VMEM((3, nx, ny, nz), F32),
            pltpu.VMEM((3 * nz, 2 * nx * ny), BF16),
            pltpu.VMEM(weights.shape, F32),
            pltpu.VMEM((nz, records), F32),
            lines, lines, lines,
            pltpu.VMEM((slots, records), BF16),
            pltpu.VMEM(populations.shape, F32),
            pltpu.VMEM((8, records), F32),
            pltpu.VMEM((5, ny, nz), F32),
            pltpu.VMEM((5, ny, nz), F32),
            edges, edges, edges, edges,
            pltpu.VMEM((4, 1, nz), F32),
            pltpu.VMEM((devices, 1, slots), F32),
            pltpu.VMEM((devices, 1, slots), F32),
            pltpu.VMEM((devices, 2 * patch[2], slots), BF16),
            pltpu.VMEM(pay, F32),
            pltpu.VMEM(pay, F32),
            pltpu.VMEM(pay, F32),
            pltpu.VMEM(pay, F32),
            pltpu.VMEM(patch, F32),
            *rim,
            pltpu.VMEM(patch, F32),
            *rim,
            pltpu.VMEM((devices, 1, LANES), F32),
            dma((4,)), dma((records // (4 * LANES),)), dma((3,)), dma((records // (4 * LANES),)),
            dma((19,)),
            to_each, to_each, to_each, to_each, to_each, to_each, to_each, to_each,
            dma((16,)), dma((16,)), to_near, to_near, to_near, to_near, to_each, to_each,
        ],
        compiler_params=pltpu.CompilerParams(collective_id=0, has_side_effects=True),
        name="couple",
    )(stiff, populations, weights, blk, own, node, modulus, live, mass)


def finish_kernel(
    parts, scal, force_ref, image_ref, backf_ref, backq_ref, blk_ref, own_ref, slot_ref,
    turned_hbm, read_hbm, out_hbm, disp_ref,
    turned, read, out, forcing, moved, turned_sem, read_sem, out_sem,
):
    devices = backf_ref.shape[0]
    depth, records = turned.shape
    _, nx, ny, nz = read.shape
    blocks = nx * ny
    slots = parts * LANES
    span = 4 * LANES
    steps = records // span
    turned_copies = [
        pltpu.make_async_copy(
            turned_hbm.at[:, pl.ds(k * span, span)], turned.at[:, pl.ds(k * span, span)],
            turned_sem.at[k],
        )
        for k in range(steps)
    ]
    stages = [
        [0] + [q for q in range(1, 19) if lattice_dirs[q][1] == 0 and lattice_dirs[q][2] == 0],
        [q for q in range(19) if lattice_dirs[q][1] != 0 and lattice_dirs[q][2] == 0],
        [q for q in range(19) if lattice_dirs[q][2] != 0],
    ]
    order = [q for stage in stages for q in stage]
    read_copies = {
        q: pltpu.make_async_copy(read_hbm.at[q], read.at[q], read_sem.at[q]) for q in order
    }
    for copy in turned_copies:
        copy.start()
    for q in order:
        read_copies[q].start()
    alpha = scal[0, 0]
    beta = scal[0, 1]
    disp_ref[...] = alpha * force_ref[...] + beta * image_ref[...]
    back = alpha * backf_ref[...] + beta * backq_ref[...]
    wide = jnp.concatenate([back[:, p * 3 : p * 3 + 3] for p in range(parts)], axis=2)
    high = wide.astype(BF16).astype(F32)
    left = jnp.concatenate([high, wide - high, jnp.zeros((devices, 2, slots), F32)], axis=1)
    left = left.reshape(devices * 8, slots).astype(BF16)

    def move_step(k, carry):
        at = pl.multiple_of(k * span, span)
        hot = (iota((slots, span), 0) == slot_ref[:, pl.ds(at, span)]).astype(F32).astype(BF16)
        found = dot_nn(left, hot)
        owners = own_ref[:, pl.ds(at, span)]
        lines = jnp.zeros((8, span), F32)
        for o in range(devices):
            lines = lines + jnp.where(owners == o, found[o * 8 : o * 8 + 8], 0.0)
        value = coupling * (lines[:3] + lines[3:6])
        moved[:, pl.ds(at, span)] = jnp.concatenate([value, jnp.zeros((5, span), F32)], axis=0)
        return carry

    lax.fori_loop(0, steps, move_step, 0)
    out_copies = {q: pltpu.make_async_copy(out.at[q], out_hbm.at[q], out_sem.at[q]) for q in order}
    for c in range(3):
        total = None
        for k in range(steps):
            if c == 0:
                turned_copies[k].wait()
            at = k * span
            hot = (iota((blocks, span), 0) == blk_ref[:, at : at + span]).astype(F32).astype(BF16)
            high, low = halves(turned[:, at : at + span] * moved[c : c + 1, at : at + span])
            part = dot_nt(
                jnp.concatenate([hot, hot], axis=1), jnp.concatenate([high, low], axis=1)
            )
            total = part if total is None else total + part
        forcing[c] = total.reshape(nx, ny, nz)
        for q in stages[c]:
            read_copies[q].wait()

            def row_step(row, carry, q=q):
                at = pl.multiple_of(row * 8, 8)
                fields = [forcing[axis_pos, pl.ds(at, 8)] if lattice_dirs[q][axis_pos] else None
                          for axis_pos in range(3)]
                projected = combine_dirs(fields, lattice_dirs[q])
                value = read[q, pl.ds(at, 8)]
                if projected is not None:
                    value = value + (3.0 * lattice_weights[q]) * projected
                out[q, pl.ds(at, 8)] = value
                return carry

            lax.fori_loop(0, nx // 8, row_step, 0)
            out_copies[q].start()
    for q in order:
        out_copies[q].wait()


def finish(parts, scal, force, image, back_f, back_q, blk, own, slot, turned, read):
    vmem = pl.BlockSpec(memory_space=pltpu.VMEM)
    hbm = pl.BlockSpec(memory_space=pl.ANY)
    records = blk.shape[1]
    steps = records // (4 * LANES)
    dma = pltpu.SemaphoreType.DMA
    return pl.pallas_call(
        functools.partial(finish_kernel, parts),
        in_specs=[pl.BlockSpec(memory_space=pltpu.SMEM)] + [vmem] * 7 + [hbm] * 2,
        out_specs=[hbm, vmem],
        out_shape=[
            jax.ShapeDtypeStruct(read.shape, F32),
            jax.ShapeDtypeStruct(force.shape, F32),
        ],
        scratch_shapes=[
            pltpu.VMEM(turned.shape, F32),
            pltpu.VMEM(read.shape, F32),
            pltpu.VMEM(read.shape, F32),
            pltpu.VMEM((3,) + read.shape[1:], F32),
            pltpu.VMEM((8, records), F32),
            dma((steps,)), dma((19,)), dma((19,)),
        ],
        name="finish",
    )(scal, force, image, back_f, back_q, blk, own, slot, turned, read)


def per_device(
    grid, populations, mass, modulus, cell_live, stiff_ref, rec_block, rec_owner, rec_node,
    rbf_weight,
):
    devices = grid[0] * grid[1]
    records = rec_block.shape[0]
    capacity = 2 * records // devices
    parts = -(-capacity // LANES)
    blk = rec_block.reshape(1, records)
    own = rec_owner.reshape(1, records)
    node = rec_node.reshape(1, records)
    read, turned, force, image, scal, slot, back_f, back_q = couple(
        grid, parts, stiff_ref, populations, rbf_weight, blk, own, node, modulus, cell_live, mass
    )
    return finish(parts, scal, force, image, back_f, back_q, blk, own, slot, turned, read)


def solution(mesh):
    grid = (mesh.shape["gx"], mesh.shape["gy"])
    in_specs = (
        P(None, "gx", "gy", None),
        P("gx", "gy"),
        P("gx", "gy"),
        P("gx", "gy"),
        P(),
        P(("gx", "gy")),
        P(("gx", "gy"), None),
        P(("gx", "gy")),
        P(("gx", "gy"), None),
    )
    out_specs = (P(None, "gx", "gy", None), P(None, "gx", "gy"))
    return jax.shard_map(
        functools.partial(per_device, grid), mesh=mesh, in_specs=in_specs, out_specs=out_specs,
        check_vma=False,
    )
```

```python
import functools
import math

import jax
import jax.numpy as jnp
from jax import lax
from jax.experimental import pallas as pl
from jax.experimental.pallas import tpu as pltpu
from jax.sharding import PartitionSpec as P

MESH = pl.DeviceIdType.MESH
F32 = jnp.float32
BF16 = jnp.bfloat16
LANES = 128

lattice_dirs = (
    (0, 0, 0),
    (1, 0, 0),
    (-1, 0, 0),
    (0, 1, 0),
    (0, -1, 0),
    (0, 0, 1),
    (0, 0, -1),
    (1, 1, 0),
    (-1, -1, 0),
    (1, -1, 0),
    (-1, 1, 0),
    (1, 0, 1),
    (-1, 0, -1),
    (1, 0, -1),
    (-1, 0, 1),
    (0, 1, 1),
    (0, -1, -1),
    (0, 1, -1),
    (0, -1, 1),
)
lattice_weights = (1.0 / 3.0,) + (1.0 / 18.0,) * 6 + (1.0 / 36.0,) * 12
relax_rate = 1.25
coupling = 0.1

x_up = [q for q in range(19) if lattice_dirs[q][0] == 1]
x_down = [q for q in range(19) if lattice_dirs[q][0] == -1]
y_up = [q for q in range(19) if lattice_dirs[q][1] == 1]
y_down = [q for q in range(19) if lattice_dirs[q][1] == -1]
diagonal = [q for q in range(19) if lattice_dirs[q][0] != 0 and lattice_dirs[q][1] != 0]


def combine_dirs(fields, direction):
    total = None
    for axis_pos in range(3):
        if direction[axis_pos] != 0:
            field = fields[axis_pos]
            if total is None:
                total = field if direction[axis_pos] == 1 else -field
            else:
                total = total + field if direction[axis_pos] == 1 else total - field
    return total


def halves(values):
    high = values.astype(BF16)
    low = (values - high.astype(F32)).astype(BF16)
    return high, low


def iota(shape, dim):
    return lax.broadcasted_iota(jnp.int32, shape, dim)


def dot_nt(left, right):
    return lax.dot_general(left, right, (((1,), (1,)), ((), ())), preferred_element_type=F32)


def dot_nn(left, right):
    return lax.dot_general(left, right, (((1,), (0,)), ((), ())), preferred_element_type=F32)


def position(grid):
    return lax.axis_index("gx"), lax.axis_index("gy")


def greet_all(grid):
    ix, iy = position(grid)
    devices = grid[0] * grid[1]
    me = ix * grid[1] + iy
    barrier = pltpu.get_barrier_semaphore()

    def signal(j, carry):
        other = lax.rem(me + j, devices)
        pl.semaphore_signal(
            barrier, inc=1, device_id=(lax.div(other, grid[1]), lax.rem(other, grid[1])),
            device_id_type=MESH,
        )
        return carry

    lax.fori_loop(1, devices, signal, 0)


def await_all(grid):
    pl.semaphore_wait(pltpu.get_barrier_semaphore(), grid[0] * grid[1] - 1)


def send_all(grid, source, target, send_sem, recv_sem):
    ix, iy = position(grid)
    devices = grid[0] * grid[1]
    me = ix * grid[1] + iy

    def body(j, carry):
        other = lax.rem(me + j, devices)
        pltpu.make_async_remote_copy(
            src_ref=source(other),
            dst_ref=target(me),
            send_sem=send_sem,
            recv_sem=recv_sem(j),
            device_id=(lax.div(other, grid[1]), lax.rem(other, grid[1])),
            device_id_type=MESH,
        ).start()
        return carry

    lax.fori_loop(1, devices, body, 0)


def neighbour_copy(grid, dx, dy, source, target, send_sem, recv_sem):
    ix, iy = position(grid)
    return pltpu.make_async_remote_copy(
        src_ref=source,
        dst_ref=target,
        send_sem=send_sem,
        recv_sem=recv_sem,
        device_id=(lax.rem(ix + dx + grid[0], grid[0]), lax.rem(iy + dy + grid[1], grid[1])),
        device_id_type=MESH,
    )


def pack_side(field, side_out):
    rows, cols = field.shape[1:]
    for c in range(3):
        tall = jnp.concatenate([field[c], jnp.zeros((cols - rows, cols), F32)], axis=0).T
        side_out[0, c] = tall[cols - 8 :]
        side_out[1, c] = tall[:8]


def rim_copies(grid, field, side_out, strip, send_sem, recv_sem):
    rows = field.shape[1]
    copies = []
    for k in range(3):
        dy = 1 - k
        copies.append(
            neighbour_copy(
                grid, 1, dy, field.at[:, pl.ds(rows - 8, 8), :], strip.at[k], send_sem, recv_sem
            )
        )
        copies.append(
            neighbour_copy(
                grid, -1, dy, field.at[:, pl.ds(0, 8), :], strip.at[3 + k], send_sem, recv_sem
            )
        )
    copies.append(neighbour_copy(grid, 0, 1, side_out.at[0], strip.at[6], send_sem, recv_sem))
    copies.append(neighbour_copy(grid, 0, -1, side_out.at[1], strip.at[7], send_sem, recv_sem))
    return copies


def settle(grid, buffer, send_sem, recv_sem):
    copy = neighbour_copy(
        grid, 0, 1, buffer, buffer, recv_sem if send_sem is None else send_sem,
        send_sem if recv_sem is None else recv_sem,
    )
    if send_sem is not None:
        copy.wait_send()
    if recv_sem is not None:
        copy.wait_recv()


def with_rim(centre, strip, c):
    rows, cols = centre.shape[1:]
    beside = jnp.concatenate([strip[7, c], jnp.zeros((cols - 16, cols), F32), strip[6, c]], axis=0)
    main = jnp.concatenate([centre[c], beside.T[:rows]], axis=1)
    low = iota((8, cols), 0) < 4
    left_strip = iota((8, cols), 1) < cols // 2
    below = jnp.where(low, strip[4, c], strip[1, c])
    corner = jnp.where(
        low,
        jnp.where(left_strip, strip[5, c], strip[3, c]),
        jnp.where(left_strip, strip[2, c], strip[0, c]),
    )
    return jnp.concatenate([main, jnp.concatenate([below, corner], axis=1)], axis=0)


def spread_rows(values, count):
    rows = jnp.broadcast_to(values, (16, values.shape[1])).astype(BF16)
    return jnp.concatenate([rows] * (count // 16), axis=0)


def one_hot(count, index):
    index = index.astype(F32)
    ramp = iota((count, index.shape[1]), 0).astype(F32).astype(BF16)
    one = jnp.ones(ramp.shape, BF16)
    return jnp.where(ramp == spread_rows(index, count), one, jnp.zeros(ramp.shape, BF16))


def owner_mask(devices, owners):
    lines = (iota((devices * 8, owners.shape[1]), 0) // 8).astype(F32).astype(BF16)
    return lines == spread_rows(owners.astype(F32), devices * 8)


def find_slots(devices, node_cols, own_ref, node_ref, slot_ref, slot_hot, node_pay):
    records = own_ref.shape[1]
    slots = slot_hot.shape[0]
    span = 2 * LANES
    steps = records // span
    before = (iota((span, span), 0) <= iota((span, span), 1)).astype(F32).astype(BF16)
    base = jnp.full((devices, span), -1.0, F32)
    routed = None
    for i in range(steps):
        hits = one_hot(devices, own_ref[:, i * span : (i + 1) * span])
        counts = dot_nn(hits, before)
        slot = jnp.sum(hits.astype(F32) * (counts + base), axis=0, keepdims=True)
        base = base + jnp.broadcast_to(counts[:, span - 1 :], (devices, span))
        slot_ref[:, i * span : (i + 1) * span] = slot.astype(jnp.int32)
        hot = one_hot(slots, slot)
        slot_hot[:, i * span : (i + 1) * span] = hot
        node = node_ref[:, i * span : (i + 1) * span]
        row = node // node_cols
        col = node - row * node_cols
        left = jnp.concatenate(
            [
                hits * spread_rows(row.astype(F32), devices),
                hits * spread_rows(col.astype(F32), devices),
            ],
            axis=0,
        )
        part = dot_nt(left, hot)
        routed = part if routed is None else routed + part
    nodes = routed[:devices] * float(node_cols) + routed[devices:]
    for o in range(devices):
        node_pay[o] = nodes[o : o + 1]


def moments(pop, mom, row):
    for axis_pos in range(3):
        total = None
        for q in range(19):
            sign = lattice_dirs[q][axis_pos]
            if sign == 1:
                total = pop[q, row] if total is None else total + pop[q, row]
            elif sign == -1:
                total = -pop[q, row] if total is None else total - pop[q, row]
        mom[axis_pos, row] = total


def collide_row(pop, mom, read, yu, yd, row):
    rows, cols, depth = read.shape[1:]
    pops = [pop[q, row] for q in range(19)]
    density = pops[0]
    for q in range(1, 19):
        density = density + pops[q]
    inverse = 1.0 / density
    velocity = [mom[axis_pos, row] * inverse for axis_pos in range(3)]
    squared = velocity[0] * velocity[0] + velocity[1] * velocity[1] + velocity[2] * velocity[2]
    rest = 1.0 - 1.5 * squared
    scaled = {w: (relax_rate * w) * density for w in sorted(set(lattice_weights))}
    ups = lax.rem(row + 1, rows)
    downs = lax.rem(row + rows - 1, rows)
    for q in range(19):
        dx, dy, dz = lattice_dirs[q]
        projected = combine_dirs(velocity, lattice_dirs[q])
        bracket = rest
        if projected is not None:
            bracket = rest + projected * (3.0 + 4.5 * projected)
        value = (1.0 - relax_rate) * pops[q] + scaled[lattice_weights[q]] * bracket
        if dz != 0:
            value = pltpu.roll(value, dz % depth, 1)
        if dy != 0:
            value = pltpu.roll(value, dy % cols, 0)
        at = ups if dx == 1 else downs if dx == -1 else row
        read[q, at] = value
        if dy == 1:
            yu[y_up.index(q), at] = value[0:1]
        if dy == -1:
            yd[y_down.index(q), at] = value[cols - 1 : cols]


def mend_edges(read, xu, xd, yu, yd, corner):
    rows, cols, depth = read.shape[1:]
    for k, q in enumerate(x_up):
        read[q, 0] = xu[k]
    for k, q in enumerate(x_down):
        read[q, rows - 1] = xd[k]

    def one(row, carry):
        for k, q in enumerate(y_up):
            read[q, row, 0:1] = yu[k, row]
        for k, q in enumerate(y_down):
            read[q, row, cols - 1 : cols] = yd[k, row]
        return carry

    lax.fori_loop(0, rows, one, 0, unroll=4)
    for k, q in enumerate(diagonal):
        dx, dy, _ = lattice_dirs[q]
        at = 0 if dy == 1 else cols - 1
        read[q, 0 if dx == 1 else rows - 1, at : at + 1] = corner[k]


def sources_of(grid, step, count):
    ix, iy = position(grid)
    devices = grid[0] * grid[1]
    me = ix * grid[1] + iy
    return [
        lax.rem(me + devices - lax.rem(step * count + d + 1, devices), devices)
        for d in range(count)
    ]


def node_parts(node, rows, cols):
    node = node.astype(jnp.int32)
    half = rows // 2 * cols
    top = node // half
    rest = node - top * half
    row = rest // cols
    return row, rest - row * cols + top * cols


def lane_row(ref, source, c, parts):
    return jnp.concatenate(
        [ref[source, p * 3 + c : p * 3 + c + 1] for p in range(parts)], axis=1
    )


def gather_force(grid, parts, node_in, node_hot, pay, force, arrived):
    ix, iy = position(grid)
    devices = pay.shape[0]
    me = ix * grid[1] + iy
    rows, cols = force.shape[1:]
    half = rows // 2
    count = math.gcd(devices, 8)
    total = None
    for step in range(devices // count):
        arrived(step)
        for d in range(count):
            source = lax.rem(me + devices - (step * count + d), devices)
            row, _ = node_parts(node_in[source], rows, cols)
            row_hot = one_hot(half, row)
            highs = []
            lows = []
            for c in range(3):
                value = lane_row(pay, source, c, parts)
                high = value.astype(BF16).astype(F32)
                highs.append(row_hot * spread_rows(high, half))
                lows.append(row_hot * spread_rows(value - high, half))
            part = dot_nt(jnp.concatenate(highs + lows, axis=0), node_hot[source])
            total = part if total is None else total + part
    total = total[: 3 * half] + total[3 * half :]
    for c in range(3):
        piece = total[c * half : (c + 1) * half]
        force[c] = jnp.concatenate([piece[:, :cols], piece[:, cols:]], axis=0)


def pick_nodes(grid, parts, field, node_in, node_hot, out, ready):
    devices = out.shape[0]
    rows, cols = field[0].shape
    half = rows // 2
    slots = parts * LANES
    count = math.gcd(devices, 8)
    wide = [jnp.concatenate([f[:half], f[half:]], axis=1) for f in field]
    high, low = halves(jnp.concatenate(wide, axis=0))
    left = jnp.concatenate([high, low], axis=0)

    def one(step, carry):
        sources = sources_of(grid, step, count)
        for source in sources:
            row, _ = node_parts(node_in[source], rows, cols)
            row_hot = iota((half, slots), 0) == row
            found = dot_nn(left, node_hot[source])
            found = found[: 3 * half] + found[3 * half :]
            values = [
                jnp.sum(
                    jnp.where(row_hot, found[c * half : (c + 1) * half], 0.0), axis=0, keepdims=True
                )
                for c in range(3)
            ]
            out[source] = jnp.concatenate(
                [value[:, p * LANES : (p + 1) * LANES] for p in range(parts) for value in values],
                axis=0,
            )
        for d in range(count):
            ready(step * count + d + 1)
        return carry

    lax.fori_loop(0, devices // count, one, 0)


def couple_kernel(
    grid, parts, stiff_hbm, pop_hbm, w_hbm, blk_hbm, own_hbm, node_hbm, modulus_hbm, live_hbm, mass_hbm,
    read, turned, force, image_buf, slot, scal_out, back_f_in, back_q_in, blk, own,
    stiff, pop, mom, mom_cat, w, node, slot_hot, loads,
    xu_in, xd_in, yu_out, yd_out, yu_in, yd_in, corner_in,
    node_pay, node_in, node_hot, pay, pay_in, back_f, back_q,
    live_in, stat, stat_out, stat_strip, side_out, strip, sums,
    pop_sem, w_sem, small_sem,
    node_sem, pay_send, pay_recv, backf_sem, backq_sem, lb_send, lb_recv, stat_sem, rim_sem, sum_sem,
):
    ix, iy = position(grid)
    devices = grid[0] * grid[1]
    me = ix * grid[1] + iy
    rows, cols = force.shape[1:]
    full = (rows + 8, 2 * cols)
    nx, ny, nz = read.shape[1:]
    blocks = nx * ny
    records = w.shape[0]
    slots = parts * LANES
    others = pl.ds(0, devices - 1)
    greet_all(grid)
    small = [
        pltpu.make_async_copy(source, target, small_sem.at[k])
        for k, (source, target) in enumerate(
            [
                (own_hbm, own), (node_hbm, node), (blk_hbm, blk), (modulus_hbm, stat.at[0]),
                (mass_hbm, stat.at[2]), (live_hbm, live_in), (stiff_hbm, stiff),
            ]
        )
    ]
    pop_rows = nx // 4
    pop_copies = [
        pltpu.make_async_copy(
            pop_hbm.at[:, pl.ds(k * pop_rows, pop_rows)], pop.at[:, pl.ds(k * pop_rows, pop_rows)],
            pop_sem.at[k],
        )
        for k in range(4)
    ]
    span = 4 * LANES
    steps = records // span

    def w_copy(k):
        at = pl.multiple_of(k * span, span)
        return pltpu.make_async_copy(w_hbm.at[pl.ds(at, span)], w.at[pl.ds(at, span)], w_sem.at[k])

    for copy in small + pop_copies:
        copy.start()
    for k in range(steps):
        w_copy(k).start()
    for copy in small[:3]:
        copy.wait()
    find_slots(devices, cols, own, node, slot, slot_hot, node_pay)

    for k, copy in enumerate(pop_copies):
        copy.wait()

        def moment_row(row, carry):
            moments(pop, mom, row)
            return carry

        lax.fori_loop(k * pop_rows, (k + 1) * pop_rows, moment_row, 0, unroll=2)
    for c in range(3):
        high, low = halves(mom[c].reshape(blocks, nz).T)
        mom_cat[c * nz : (c + 1) * nz, :blocks] = high
        mom_cat[c * nz : (c + 1) * nz, blocks:] = low
    await_all(grid)
    send_all(
        grid, lambda o: node_pay.at[o], lambda m: node_in.at[m], node_sem.at[0],
        lambda j: node_sem.at[1],
    )
    node_in[me] = node_pay[me]

    def load_step(k, carry):
        w_copy(k).wait()
        at = pl.multiple_of(k * span, span)
        hot = one_hot(blocks, blk[:, pl.ds(at, span)])
        picked = dot_nn(mom_cat[...], jnp.concatenate([hot, hot], axis=0))
        flipped = w[pl.ds(at, span), :].T
        turned[:, pl.ds(at, span)] = flipped
        highs = []
        lows = []
        for c in range(3):
            load = jnp.sum(picked[c * nz : (c + 1) * nz] * flipped, axis=0, keepdims=True)
            high = load.astype(BF16).astype(F32)
            highs.append(high)
            lows.append(load - high)
        loads[:, pl.ds(at, span)] = jnp.concatenate(
            highs + lows + [jnp.zeros((2, span), F32)], axis=0
        )
        return carry

    lax.fori_loop(0, steps, load_step, 0)
    routed = None
    for k in range(steps):
        at = k * span
        value = loads[:, at : at + span]
        value = jnp.concatenate([value, value], axis=0).astype(BF16)
        value = jnp.concatenate([value] * (devices // 2), axis=0)
        spread = jnp.where(
            owner_mask(devices, own[:, at : at + span]), value, jnp.zeros(value.shape, BF16)
        )
        part = dot_nt(spread, slot_hot[:, at : at + span])
        routed = part if routed is None else routed + part
    for o in range(devices):
        tile = routed[o * 8 : o * 8 + 3] + routed[o * 8 + 3 : o * 8 + 6]
        pay[o] = jnp.concatenate(
            [tile[:, p * LANES : (p + 1) * LANES] for p in range(parts)], axis=0
        )
    batch = math.gcd(devices, 8)
    send_all(
        grid, lambda o: pay.at[o], lambda m: pay_in.at[m], pay_send.at[0],
        lambda j: pay_recv.at[lax.div(j, batch)],
    )
    pay_in[me] = pay[me]
    for copy in small[3:]:
        copy.wait()
    stat[1] = live_in[...].astype(F32)
    pack_side(stat, stat_out)
    for copy in rim_copies(grid, stat, stat_out, stat_strip, stat_sem.at[0], stat_sem.at[1]):
        copy.start()

    settle(grid, node_in.at[others], node_sem.at[0], node_sem.at[1])

    def hot_step(d, carry):
        _, col = node_parts(node_in[d], rows, cols)
        node_hot[d] = one_hot(2 * cols, col)
        return carry

    lax.fori_loop(0, devices, hot_step, 0, unroll=4)

    def collide_step(row, carry):
        collide_row(pop, mom, read, yu_out, yd_out, row)
        return carry

    lax.fori_loop(0, nx, collide_step, 0, unroll=2)
    lb_copies = []

    def lb_copy(number, dx, dy, source, target):
        lb_copies.append(
            neighbour_copy(grid, dx, dy, source, target, lb_send.at[number], lb_recv.at[number])
        )

    for k, q in enumerate(x_up):
        lb_copy(0, 1, 0, read.at[q, 0], xu_in.at[k])
    for k, q in enumerate(x_down):
        lb_copy(1, -1, 0, read.at[q, nx - 1], xd_in.at[k])
    for k, q in enumerate(diagonal):
        dx, dy, _ = lattice_dirs[q]
        edge = yu_out.at[y_up.index(q)] if dy == 1 else yd_out.at[y_down.index(q)]
        lb_copy(2, dx, dy, edge.at[0 if dx == 1 else nx - 1], corner_in.at[k])
    lb_copy(3, 0, 1, yu_out, yu_in)
    lb_copy(4, 0, -1, yd_out, yd_in)

    def pay_arrived(step):
        got = batch - 1 if step == 0 else batch
        settle(grid, pay_in.at[pl.ds(0, got)], None, pay_recv.at[step])

    gather_force(grid, parts, node_in, node_hot, pay_in, force, pay_arrived)
    pack_side(force, side_out)
    for copy in rim_copies(grid, force, side_out, strip, rim_sem.at[0], rim_sem.at[1]) + lb_copies:
        copy.start()

    def sender(back, back_in, sem):
        def ready(j):
            @pl.when(j < devices)
            def _():
                other = lax.rem(me + devices - j, devices)
                pltpu.make_async_remote_copy(
                    src_ref=back.at[other],
                    dst_ref=back_in.at[me],
                    send_sem=sem.at[0],
                    recv_sem=sem.at[1],
                    device_id=(lax.div(other, grid[1]), lax.rem(other, grid[1])),
                    device_id_type=MESH,
                ).start()

        return ready

    pick_nodes(
        grid, parts, [force[c] for c in range(3)], node_in, node_hot, back_f,
        sender(back_f, back_f_in, backf_sem),
    )
    back_f_in[me] = back_f[me]

    def back_row(a):
        return pltpu.roll(a, full[0] - 1, 0)

    def back_col(a):
        return pltpu.roll(a, full[1] - 1, 1)

    settle(grid, stat_strip, stat_sem.at[0], stat_sem.at[1])
    moduli = with_rim(stat, stat_strip, 0)
    live = with_rim(stat, stat_strip, 1)
    mass = with_rim(stat, stat_strip, 2)
    next_row = back_row(moduli)
    scale = live * (moduli + next_row + back_col(moduli) + back_col(next_row)) * 0.25

    def operate(fields):
        down = [back_row(f) for f in fields]
        corners = (
            list(fields) + down + [back_col(f) for f in fields] + [back_col(f) for f in down]
        )
        results = []
        for k in range(12):
            total = stiff[k, 0] * corners[0]
            for l in range(1, 12):
                total = total + stiff[k, l] * corners[l]
            results.append(scale * total)
        images = []
        for c in range(3):
            right = results[6 + c] + pltpu.roll(results[9 + c], 1, 0)
            images.append(
                mass * fields[c]
                + results[c]
                + pltpu.roll(results[3 + c], 1, 0)
                + pltpu.roll(right, 1, 1)
            )
        return images

    def inner(a, b):
        total = a[0] * b[0]
        for c in range(1, 3):
            total = total + a[c] * b[c]
        return jnp.sum(jnp.sum(total, axis=0, keepdims=True), axis=1, keepdims=True)

    settle(grid, strip, rim_sem.at[0], rim_sem.at[1])
    field = [with_rim(force, strip, c) for c in range(3)]
    image = operate(field)
    f = [a[:rows, :cols] for a in field]
    q = [a[:rows, :cols] for a in image]
    for c in range(3):
        image_buf[c] = q[c]
    pick_nodes(grid, parts, q, node_in, node_hot, back_q, sender(back_q, back_q_in, backq_sem))
    back_q_in[me] = back_q[me]
    second = operate(image)
    s = [a[:rows, :cols] for a in second]
    ff, fq, qq, qs = inner(f, f), inner(f, q), inner(q, q), inner(q, s)
    guess = jnp.where(qq > 0.0, fq / jnp.where(qq > 0.0, qq, 1.0), 0.0)
    r0 = [f[c] - guess * q[c] for c in range(3)]
    u0 = [q[c] - guess * s[c] for c in range(3)]
    mine = [
        ff, fq, qq, qs, guess, inner(r0, r0), inner(r0, q), inner(r0, u0), inner(r0, s), inner(q, u0)
    ]
    lane = iota((1, LANES), 1)
    line = jnp.zeros((1, LANES), F32)
    for k, value in enumerate(mine):
        line = jnp.where(lane == k, value, line)
    sums[me] = line
    send_all(
        grid, lambda o: sums.at[me], lambda m: sums.at[m], sum_sem.at[0], lambda j: sum_sem.at[1]
    )

    settle(grid, xu_in, lb_send.at[0], lb_recv.at[0])
    settle(grid, xd_in, lb_send.at[1], lb_recv.at[1])
    settle(grid, corner_in, lb_send.at[2], lb_recv.at[2])
    settle(grid, yu_in, lb_send.at[3], lb_recv.at[3])
    settle(grid, yd_in, lb_send.at[4], lb_recv.at[4])
    mend_edges(read, xu_in, xd_in, yu_in, yd_in, corner_in)
    settle(grid, sums.at[others], sum_sem.at[0], sum_sem.at[1])
    every = sums[...].reshape(devices, LANES)
    ff, fq, qq, qs, guess, r0r0, r0q, r0u0, r0s, qu0 = [
        every[:, k : k + 1] for k in range(len(mine))
    ]

    def total(value):
        return jnp.sum(value, axis=0, keepdims=True)

    ff_all, fq_all = total(ff), total(fq)
    first = ff_all / fq_all
    off = guess - first
    rr = total(r0r0 + off * (2.0 * r0q + off * qq))
    rs = total(r0u0 + off * (r0s + qu0 + off * qs))
    rq = total(r0q + off * qq)
    ratio = rr / ff_all
    step_two = rr / (rs + 2.0 * ratio * rq + ratio * ratio * fq_all)
    alpha = first + step_two * (1.0 + ratio)
    beta = -(step_two * first)
    scal_out[0:1] = jnp.broadcast_to(alpha, (1, LANES))
    scal_out[1:2] = jnp.broadcast_to(beta, (1, LANES))
    settle(grid, pay.at[others], pay_send.at[0], None)
    settle(grid, back_f_in.at[others], backf_sem.at[0], backf_sem.at[1])
    settle(grid, back_q_in.at[others], backq_sem.at[0], backq_sem.at[1])


def couple(grid, parts, stiff, populations, weights, blk, own, node, modulus, live, mass):
    devices = grid[0] * grid[1]
    _, nx, ny, nz = populations.shape
    records = weights.shape[0]
    patch = (3,) + mass.shape
    slots = parts * LANES
    vmem = pl.BlockSpec(memory_space=pltpu.VMEM)
    hbm = pl.BlockSpec(memory_space=pltpu.HBM)
    rim = [pltpu.VMEM((2, 3, 8, patch[2]), F32), pltpu.VMEM((8, 3, 8, patch[2]), F32)]
    pay = (devices, 3 * parts, LANES)
    back = jax.ShapeDtypeStruct(pay, F32)
    dma = pltpu.SemaphoreType.DMA
    lines = pltpu.VMEM((1, records), jnp.int32)
    edges = pltpu.VMEM((5, nx, 1, nz), F32)
    return pl.pallas_call(
        functools.partial(couple_kernel, grid, parts),
        in_specs=[hbm] * 9,
        out_specs=[vmem] * 10,
        out_shape=[
            jax.ShapeDtypeStruct(populations.shape, F32),
            jax.ShapeDtypeStruct((nz, records), F32),
            jax.ShapeDtypeStruct(patch, F32),
            jax.ShapeDtypeStruct(patch, F32),
            jax.ShapeDtypeStruct((1, records), jnp.int32),
            jax.ShapeDtypeStruct((2, LANES), F32),
            back,
            back,
            jax.ShapeDtypeStruct((1, records), jnp.int32),
            jax.ShapeDtypeStruct((1, records), jnp.int32),
        ],
        scratch_shapes=[
            pltpu.SMEM(stiff.shape, F32),
            pltpu.VMEM(populations.shape, F32),
            pltpu.VMEM((3, nx, ny, nz), F32),
            pltpu.VMEM((3 * nz, 2 * nx * ny), BF16),
            pltpu.VMEM(weights.shape, F32),
            lines,
            pltpu.VMEM((slots, records), BF16),
            pltpu.VMEM((8, records), F32),
            pltpu.VMEM((5, ny, nz), F32),
            pltpu.VMEM((5, ny, nz), F32),
            edges, edges, edges, edges,
            pltpu.VMEM((4, 1, nz), F32),
            pltpu.VMEM((devices, 1, slots), F32),
            pltpu.VMEM((devices, 1, slots), F32),
            pltpu.VMEM((devices, 2 * patch[2], slots), BF16),
            pltpu.VMEM(pay, F32),
            pltpu.VMEM(pay, F32),
            pltpu.VMEM(pay, F32),
            pltpu.VMEM(pay, F32),
            pltpu.VMEM(mass.shape, jnp.int32),
            pltpu.VMEM(patch, F32),
            *rim,
            *rim,
            pltpu.VMEM((devices, 1, LANES), F32),
            dma((4,)), dma((records // (4 * LANES),)), dma((7,)),
            dma((2,)), dma((1,)), dma((devices // math.gcd(devices, 8),)), dma((2,)), dma((2,)),
            dma((5,)), dma((5,)), dma((2,)), dma((2,)), dma((2,)),
        ],
        compiler_params=pltpu.CompilerParams(
            collective_id=0, has_side_effects=True, vmem_limit_bytes=36 * 2**20
        ),
        name="couple",
    )(stiff, populations, weights, blk, own, node, modulus, live, mass)


def finish_kernel(
    parts, scal, force, image, backf, backq, blk, own, slot, turned, read,
    out_hbm, disp_hbm,
    out, block_hot, forcing, moved, disp, out_sem,
):
    devices = backf.shape[0]
    depth, records = turned.shape
    _, nx, ny, nz = read.shape
    blocks = nx * ny
    slots = parts * LANES
    span = 4 * LANES
    steps = records // span
    stages = [
        [q for q in range(1, 19) if lattice_dirs[q][1] == 0 and lattice_dirs[q][2] == 0],
        [q for q in range(19) if lattice_dirs[q][1] != 0 and lattice_dirs[q][2] == 0],
        [q for q in range(19) if lattice_dirs[q][2] != 0],
    ]
    out_copies = [
        pltpu.make_async_copy(out.at[q], out_hbm.at[q], out_sem.at[q]) for q in range(19)
    ]
    alpha = scal[0:1]
    beta = scal[1:2]

    def rest_step(row, carry):
        out[0, row] = read[0, row]
        return carry

    lax.fori_loop(0, nx, rest_step, 0, unroll=4)
    out_copies[0].start()
    for c in range(3):
        disp[c] = alpha * force[c] + beta * image[c]
    disp_copy = pltpu.make_async_copy(disp, disp_hbm, out_sem.at[19])
    disp_copy.start()
    back = alpha.reshape(1, 1, LANES) * backf[...] + beta.reshape(1, 1, LANES) * backq[...]
    wide = jnp.concatenate([back[:, p * 3 : p * 3 + 3] for p in range(parts)], axis=2)
    high = wide.astype(BF16).astype(F32)
    left = jnp.concatenate([high, wide - high, jnp.zeros((devices, 2, slots), F32)], axis=1)
    left = left.reshape(devices * 8, slots).astype(BF16)

    def move_step(k, carry):
        at = pl.multiple_of(k * span, span)
        found = dot_nn(left, one_hot(slots, slot[:, pl.ds(at, span)]))
        owners = own[:, pl.ds(at, span)]
        lines = [jnp.zeros((8, span), F32) for _ in range(4)]
        for o in range(devices):
            lines[o % 4] = lines[o % 4] + jnp.where(owners == o, found[o * 8 : o * 8 + 8], 0.0)
        lines = (lines[0] + lines[1]) + (lines[2] + lines[3])
        value = coupling * (lines[:3] + lines[3:6])
        moved[:, pl.ds(at, span)] = jnp.concatenate([value, jnp.zeros((5, span), F32)], axis=0)
        block_hot[:, pl.ds(at, span)] = one_hot(blocks, blk[:, pl.ds(at, span)])
        return carry

    lax.fori_loop(0, steps, move_step, 0)
    for c in range(3):
        total = None
        for k in range(steps):
            at = k * span
            hot = block_hot[:, at : at + span]
            high, low = halves(turned[:, at : at + span] * moved[c : c + 1, at : at + span])
            part = dot_nt(jnp.concatenate([high, low], axis=0), hot)
            total = part if total is None else total + part
        forcing[c] = (total[:depth] + total[depth:]).T.reshape(nx, ny, nz)

        def row_step(row, carry, c=c):
            fields = [forcing[axis_pos, row] if axis_pos <= c else None for axis_pos in range(3)]
            for q in stages[c]:
                projected = combine_dirs(fields, lattice_dirs[q])
                out[q, row] = read[q, row] + (3.0 * lattice_weights[q]) * projected
            return carry

        lax.fori_loop(0, nx, row_step, 0, unroll=2)
        for q in stages[c]:
            out_copies[q].start()
    disp_copy.wait()
    for copy in out_copies:
        copy.wait()


def finish(parts, scal, force, image, back_f, back_q, blk, own, slot, turned, read):
    hbm = pl.BlockSpec(memory_space=pltpu.HBM)
    vmem = pl.BlockSpec(memory_space=pltpu.VMEM)
    records = blk.shape[1]
    dma = pltpu.SemaphoreType.DMA
    return pl.pallas_call(
        functools.partial(finish_kernel, parts),
        in_specs=[vmem] * 10,
        out_specs=[hbm, hbm],
        out_shape=[
            jax.ShapeDtypeStruct(read.shape, F32),
            jax.ShapeDtypeStruct(force.shape, F32),
        ],
        scratch_shapes=[
            pltpu.VMEM(read.shape, F32),
            pltpu.VMEM((read.shape[1] * read.shape[2], records), BF16),
            pltpu.VMEM((3,) + read.shape[1:], F32),
            pltpu.VMEM((8, records), F32),
            pltpu.VMEM(force.shape, F32),
            dma((20,)),
        ],
        compiler_params=pltpu.CompilerParams(vmem_limit_bytes=24 * 2**20),
        name="finish",
    )(scal, force, image, back_f, back_q, blk, own, slot, turned, read)


def per_device(
    grid, populations, mass, modulus, cell_live, stiff_ref, rec_block, rec_owner, rec_node,
    rbf_weight,
):
    devices = grid[0] * grid[1]
    records = rec_block.shape[0]
    capacity = 2 * records // devices
    parts = -(-capacity // LANES)
    blk = rec_block.reshape(1, records)
    own = rec_owner.reshape(1, records)
    node = rec_node.reshape(1, records)
    operands = [
        pltpu.with_memory_space_constraint(a, pltpu.HBM)
        for a in (stiff_ref, populations, rbf_weight, blk, own, node, modulus, cell_live, mass)
    ]
    read, turned, force, image, slot, scal, back_f, back_q, held_blk, held_own = couple(
        grid, parts, *operands
    )
    return finish(
        parts, scal, force, image, back_f, back_q, held_blk, held_own, slot, turned, read
    )


def solution(mesh):
    grid = (mesh.shape["gx"], mesh.shape["gy"])
    in_specs = (
        P(None, "gx", "gy", None),
        P("gx", "gy"),
        P("gx", "gy"),
        P("gx", "gy"),
        P(),
        P(("gx", "gy")),
        P(("gx", "gy"), None),
        P(("gx", "gy")),
        P(("gx", "gy"), None),
    )
    out_specs = (P(None, "gx", "gy", None), P(None, "gx", "gy"))
    return jax.shard_map(
        functools.partial(per_device, grid), mesh=mesh, in_specs=in_specs, out_specs=out_specs,
        check_vma=False,
    )
```

```python
import functools
import math

import jax
import jax.numpy as jnp
from jax import lax
from jax.experimental import pallas as pl
from jax.experimental.pallas import tpu as pltpu
from jax.sharding import PartitionSpec as P

MESH = pl.DeviceIdType.MESH
F32 = jnp.float32
BF16 = jnp.bfloat16
LANES = 128

lattice_dirs = (
    (0, 0, 0),
    (1, 0, 0),
    (-1, 0, 0),
    (0, 1, 0),
    (0, -1, 0),
    (0, 0, 1),
    (0, 0, -1),
    (1, 1, 0),
    (-1, -1, 0),
    (1, -1, 0),
    (-1, 1, 0),
    (1, 0, 1),
    (-1, 0, -1),
    (1, 0, -1),
    (-1, 0, 1),
    (0, 1, 1),
    (0, -1, -1),
    (0, 1, -1),
    (0, -1, 1),
)
lattice_weights = (1.0 / 3.0,) + (1.0 / 18.0,) * 6 + (1.0 / 36.0,) * 12
relax_rate = 1.25
coupling = 0.1

x_up = [q for q in range(19) if lattice_dirs[q][0] == 1]
x_down = [q for q in range(19) if lattice_dirs[q][0] == -1]
y_up = [q for q in range(19) if lattice_dirs[q][1] == 1]
y_down = [q for q in range(19) if lattice_dirs[q][1] == -1]
diagonal = [q for q in range(19) if lattice_dirs[q][0] != 0 and lattice_dirs[q][1] != 0]


def combine_dirs(fields, direction):
    total = None
    for axis_pos in range(3):
        if direction[axis_pos] != 0:
            field = fields[axis_pos]
            if total is None:
                total = field if direction[axis_pos] == 1 else -field
            else:
                total = total + field if direction[axis_pos] == 1 else total - field
    return total


def halves(values):
    high = values.astype(BF16)
    low = (values - high.astype(F32)).astype(BF16)
    return high, low


def iota(shape, dim):
    return lax.broadcasted_iota(jnp.int32, shape, dim)


def dot_nt(left, right):
    return lax.dot_general(left, right, (((1,), (1,)), ((), ())), preferred_element_type=F32)


def dot_nn(left, right):
    return lax.dot_general(left, right, (((1,), (0,)), ((), ())), preferred_element_type=F32)


def position(grid):
    return lax.axis_index("gx"), lax.axis_index("gy")


def greet_all(grid):
    ix, iy = position(grid)
    devices = grid[0] * grid[1]
    me = ix * grid[1] + iy
    barrier = pltpu.get_barrier_semaphore()

    def signal(j, carry):
        other = lax.rem(me + j, devices)
        pl.semaphore_signal(
            barrier, inc=1, device_id=(lax.div(other, grid[1]), lax.rem(other, grid[1])),
            device_id_type=MESH,
        )
        return carry

    lax.fori_loop(1, devices, signal, 0)


def await_all(grid):
    pl.semaphore_wait(pltpu.get_barrier_semaphore(), grid[0] * grid[1] - 1)


def send_all(grid, source, target, send_sem, recv_sem):
    ix, iy = position(grid)
    devices = grid[0] * grid[1]
    me = ix * grid[1] + iy

    def body(j, carry):
        other = lax.rem(me + j, devices)
        pltpu.make_async_remote_copy(
            src_ref=source(other),
            dst_ref=target(me),
            send_sem=send_sem,
            recv_sem=recv_sem(j),
            device_id=(lax.div(other, grid[1]), lax.rem(other, grid[1])),
            device_id_type=MESH,
        ).start()
        return carry

    lax.fori_loop(1, devices, body, 0)


def neighbour_copy(grid, dx, dy, source, target, send_sem, recv_sem):
    ix, iy = position(grid)
    return pltpu.make_async_remote_copy(
        src_ref=source,
        dst_ref=target,
        send_sem=send_sem,
        recv_sem=recv_sem,
        device_id=(lax.rem(ix + dx + grid[0], grid[0]), lax.rem(iy + dy + grid[1], grid[1])),
        device_id_type=MESH,
    )


def pack_side(field, side_out):
    rows, cols = field.shape[1:]
    for c in range(3):
        tall = jnp.concatenate([field[c], jnp.zeros((cols - rows, cols), F32)], axis=0).T
        side_out[0, c] = tall[cols - 8 :]
        side_out[1, c] = tall[:8]


def rim_copies(grid, field, side_out, strip, send_sem, recv_sem):
    rows = field.shape[1]
    copies = []
    for k in range(3):
        dy = 1 - k
        copies.append(
            neighbour_copy(
                grid, 1, dy, field.at[:, pl.ds(rows - 8, 8), :], strip.at[k], send_sem, recv_sem
            )
        )
        copies.append(
            neighbour_copy(
                grid, -1, dy, field.at[:, pl.ds(0, 8), :], strip.at[3 + k], send_sem, recv_sem
            )
        )
    copies.append(neighbour_copy(grid, 0, 1, side_out.at[0], strip.at[6], send_sem, recv_sem))
    copies.append(neighbour_copy(grid, 0, -1, side_out.at[1], strip.at[7], send_sem, recv_sem))
    return copies


def settle(grid, buffer, send_sem, recv_sem):
    copy = neighbour_copy(
        grid, 0, 1, buffer, buffer, recv_sem if send_sem is None else send_sem,
        send_sem if recv_sem is None else recv_sem,
    )
    if send_sem is not None:
        copy.wait_send()
    if recv_sem is not None:
        copy.wait_recv()


def with_rim(centre, strip, c):
    rows, cols = centre.shape[1:]
    beside = jnp.concatenate([strip[7, c], jnp.zeros((cols - 16, cols), F32), strip[6, c]], axis=0)
    main = jnp.concatenate([centre[c], beside.T[:rows]], axis=1)
    low = iota((8, cols), 0) < 4
    left_strip = iota((8, cols), 1) < cols // 2
    below = jnp.where(low, strip[4, c], strip[1, c])
    corner = jnp.where(
        low,
        jnp.where(left_strip, strip[5, c], strip[3, c]),
        jnp.where(left_strip, strip[2, c], strip[0, c]),
    )
    return jnp.concatenate([main, jnp.concatenate([below, corner], axis=1)], axis=0)


def spread_rows(values, count):
    rows = jnp.broadcast_to(values, (16, values.shape[1])).astype(BF16)
    return jnp.concatenate([rows] * (count // 16), axis=0)


def one_hot(count, index):
    index = index.astype(F32)
    ramp = iota((count, index.shape[1]), 0).astype(F32).astype(BF16)
    one = jnp.ones(ramp.shape, BF16)
    return jnp.where(ramp == spread_rows(index, count), one, jnp.zeros(ramp.shape, BF16))


def add_to(chains, number, part):
    held = chains[number]
    chains[number] = part if held is None else held + part


def owner_mask(devices, owners):
    lines = (iota((devices * 8, owners.shape[1]), 0) // 8).astype(F32).astype(BF16)
    return lines == spread_rows(owners.astype(F32), devices * 8)


def find_slots(devices, node_cols, own_ref, node_ref, slot_hot, node_pay):
    records = own_ref.shape[1]
    slots = slot_hot.shape[0]
    span = 2 * LANES
    steps = records // span
    before = (iota((span, span), 0) <= iota((span, span), 1)).astype(F32).astype(BF16)
    base = jnp.full((devices, span), -1.0, F32)
    routed = None
    for i in range(steps):
        hits = one_hot(devices, own_ref[:, i * span : (i + 1) * span])
        counts = dot_nn(hits, before)
        slot = jnp.sum(hits.astype(F32) * (counts + base), axis=0, keepdims=True)
        base = base + jnp.broadcast_to(counts[:, span - 1 :], (devices, span))
        hot = one_hot(slots, slot)
        slot_hot[:, i * span : (i + 1) * span] = hot
        node = node_ref[:, i * span : (i + 1) * span]
        row = node // node_cols
        col = node - row * node_cols
        left = jnp.concatenate(
            [
                hits * spread_rows(row.astype(F32), devices),
                hits * spread_rows(col.astype(F32), devices),
            ],
            axis=0,
        )
        part = dot_nt(left, hot)
        routed = part if routed is None else routed + part
    nodes = routed[:devices] * float(node_cols) + routed[devices:]
    for o in range(devices):
        node_pay[o] = nodes[o : o + 1]


def moments(pop, mom, row):
    for axis_pos in range(3):
        total = None
        for q in range(19):
            sign = lattice_dirs[q][axis_pos]
            if sign == 1:
                total = pop[q, row] if total is None else total + pop[q, row]
            elif sign == -1:
                total = -pop[q, row] if total is None else total - pop[q, row]
        mom[axis_pos, row] = total


def collide_row(pop, mom, read, yu, yd, row):
    rows, cols, depth = read.shape[1:]
    pops = [pop[q, row] for q in range(19)]
    density = pops[0]
    for q in range(1, 19):
        density = density + pops[q]
    inverse = 1.0 / density
    velocity = [mom[axis_pos, row] * inverse for axis_pos in range(3)]
    squared = velocity[0] * velocity[0] + velocity[1] * velocity[1] + velocity[2] * velocity[2]
    rest = 1.0 - 1.5 * squared
    scaled = {w: (relax_rate * w) * density for w in sorted(set(lattice_weights))}
    ups = lax.rem(row + 1, rows)
    downs = lax.rem(row + rows - 1, rows)
    for q in range(19):
        dx, dy, dz = lattice_dirs[q]
        projected = combine_dirs(velocity, lattice_dirs[q])
        bracket = rest
        if projected is not None:
            bracket = rest + projected * (3.0 + 4.5 * projected)
        value = (1.0 - relax_rate) * pops[q] + scaled[lattice_weights[q]] * bracket
        if dz != 0:
            value = pltpu.roll(value, dz % depth, 1)
        if dy != 0:
            value = pltpu.roll(value, dy % cols, 0)
        at = ups if dx == 1 else downs if dx == -1 else row
        read[q, at] = value
        if dy == 1:
            yu[y_up.index(q), at] = value[0:1]
        if dy == -1:
            yd[y_down.index(q), at] = value[cols - 1 : cols]


def mend_edges(read, xu, xd, yu, yd, corner):
    rows, cols, depth = read.shape[1:]
    for k, q in enumerate(x_up):
        read[q, 0] = xu[k]
    for k, q in enumerate(x_down):
        read[q, rows - 1] = xd[k]

    def one(row, carry):
        for k, q in enumerate(y_up):
            read[q, row, 0:1] = yu[k, row]
        for k, q in enumerate(y_down):
            read[q, row, cols - 1 : cols] = yd[k, row]
        return carry

    lax.fori_loop(0, rows, one, 0, unroll=4)
    for k, q in enumerate(diagonal):
        dx, dy, _ = lattice_dirs[q]
        at = 0 if dy == 1 else cols - 1
        read[q, 0 if dx == 1 else rows - 1, at : at + 1] = corner[k]


def sources_of(grid, step, count):
    ix, iy = position(grid)
    devices = grid[0] * grid[1]
    me = ix * grid[1] + iy
    return [
        lax.rem(me + devices - lax.rem(step * count + d + 1, devices), devices)
        for d in range(count)
    ]


def node_parts(node, rows, cols):
    node = node.astype(jnp.int32)
    half = rows // 2 * cols
    top = node // half
    rest = node - top * half
    row = rest // cols
    return row, rest - row * cols + top * cols


def lane_row(ref, source, c, parts):
    return jnp.concatenate(
        [ref[source, p * 3 + c : p * 3 + c + 1] for p in range(parts)], axis=1
    )


def gather_force(grid, parts, node_in, node_hot, pay, force, arrived):
    ix, iy = position(grid)
    devices = pay.shape[0]
    me = ix * grid[1] + iy
    rows, cols = force.shape[1:]
    half = rows // 2
    count = math.gcd(devices, 8)
    chains = [None, None]
    for step in range(devices // count):
        arrived(step)
        for d in range(count):
            source = lax.rem(me + devices - (step * count + d), devices)
            row, _ = node_parts(node_in[source], rows, cols)
            row_hot = one_hot(half, row)
            highs = []
            lows = []
            for c in range(3):
                value = lane_row(pay, source, c, parts)
                high = value.astype(BF16).astype(F32)
                highs.append(row_hot * spread_rows(high, half))
                lows.append(row_hot * spread_rows(value - high, half))
            for number in range(2):
                lines = slice(number * half // 2, (number + 1) * half // 2)
                left = jnp.concatenate([piece[lines] for piece in highs + lows], axis=0)
                add_to(chains, number, dot_nt(left, node_hot[source]))
    middle = half // 2
    chains = [chain[: 3 * middle] + chain[3 * middle :] for chain in chains]
    for c in range(3):
        piece = jnp.concatenate(
            [chain[c * middle : (c + 1) * middle] for chain in chains], axis=0
        )
        force[c] = jnp.concatenate([piece[:, :cols], piece[:, cols:]], axis=0)


def pick_nodes(grid, parts, field, node_in, node_hot, out, ready):
    devices = out.shape[0]
    rows, cols = field[0].shape
    half = rows // 2
    slots = parts * LANES
    count = math.gcd(devices, 8)
    wide = [jnp.concatenate([f[:half], f[half:]], axis=1) for f in field]
    high, low = halves(jnp.concatenate(wide, axis=0))
    left = jnp.concatenate([high, low], axis=0)

    def one(step, carry):
        sources = sources_of(grid, step, count)
        for source in sources:
            row, _ = node_parts(node_in[source], rows, cols)
            row_hot = iota((half, slots), 0) == row
            found = dot_nn(left, node_hot[source])
            found = found[: 3 * half] + found[3 * half :]
            values = [
                jnp.sum(
                    jnp.where(row_hot, found[c * half : (c + 1) * half], 0.0), axis=0, keepdims=True
                )
                for c in range(3)
            ]
            out[source] = jnp.concatenate(
                [value[:, p * LANES : (p + 1) * LANES] for p in range(parts) for value in values],
                axis=0,
            )
        for d in range(count):
            ready(step * count + d + 1)
        return carry

    lax.fori_loop(0, devices // count, one, 0)


def couple_kernel(
    grid, parts, stiff_hbm, pop_hbm, w_hbm, blk_hbm, own_hbm, node_hbm, modulus_hbm, live_hbm, mass_hbm,
    read, turned, force, image_buf, slot_hot, hot_turned, scal_out, back_f_in, back_q_in, own,
    stiff, pop, mom, mom_cat, w, node, blk, loads,
    xu_in, xd_in, yu_out, yd_out, yu_in, yd_in, corner_in,
    node_pay, node_in, node_hot, pay, pay_in, back_f, back_q,
    live_in, stat, stat_out, stat_strip, side_out, strip, sums,
    pop_sem, w_sem, small_sem,
    node_sem, pay_send, pay_recv, backf_sem, backq_sem, lb_send, lb_recv, stat_sem, rim_sem, sum_sem,
):
    ix, iy = position(grid)
    devices = grid[0] * grid[1]
    me = ix * grid[1] + iy
    rows, cols = force.shape[1:]
    full = (rows + 8, 2 * cols)
    nx, ny, nz = read.shape[1:]
    blocks = nx * ny
    records = w.shape[0]
    slots = parts * LANES
    others = pl.ds(0, devices - 1)
    greet_all(grid)
    small = [
        pltpu.make_async_copy(source, target, small_sem.at[k])
        for k, (source, target) in enumerate(
            [
                (own_hbm, own), (node_hbm, node), (blk_hbm, blk), (modulus_hbm, stat.at[0]),
                (mass_hbm, stat.at[2]), (live_hbm, live_in), (stiff_hbm, stiff),
            ]
        )
    ]
    pop_rows = nx // 4
    pop_copies = [
        pltpu.make_async_copy(
            pop_hbm.at[:, pl.ds(k * pop_rows, pop_rows)], pop.at[:, pl.ds(k * pop_rows, pop_rows)],
            pop_sem.at[k],
        )
        for k in range(4)
    ]
    span = 4 * LANES
    steps = records // span

    def w_copy(k):
        at = pl.multiple_of(k * span, span)
        return pltpu.make_async_copy(w_hbm.at[pl.ds(at, span)], w.at[pl.ds(at, span)], w_sem.at[k])

    for copy in small + pop_copies:
        copy.start()
    for copy in small[:3]:
        copy.wait()
    find_slots(devices, cols, own, node, slot_hot, node_pay)

    for k, copy in enumerate(pop_copies):
        copy.wait()
        if k == 1:
            for number in range(steps):
                w_copy(number).start()

        def moment_row(row, carry):
            moments(pop, mom, row)
            return carry

        lax.fori_loop(k * pop_rows, (k + 1) * pop_rows, moment_row, 0, unroll=2)
    for c in range(3):
        high, low = halves(mom[c].reshape(blocks, nz).T)
        mom_cat[c * nz : (c + 1) * nz, :blocks] = high
        mom_cat[c * nz : (c + 1) * nz, blocks:] = low
    for copy in small[3:]:
        copy.wait()
    stat[1] = live_in[...].astype(F32)
    pack_side(stat, stat_out)
    await_all(grid)
    send_all(
        grid, lambda o: node_pay.at[o], lambda m: node_in.at[m], node_sem.at[0],
        lambda j: node_sem.at[1],
    )
    node_in[me] = node_pay[me]
    for copy in rim_copies(grid, stat, stat_out, stat_strip, stat_sem.at[0], stat_sem.at[1]):
        copy.start()

    def load_step(k, carry):
        w_copy(k).wait()
        at = pl.multiple_of(k * span, span)
        hot = one_hot(blocks, blk[:, pl.ds(at, span)])
        picked = dot_nn(mom_cat[...], jnp.concatenate([hot, hot], axis=0))
        flipped = w[pl.ds(at, span), :].T
        turned[:, pl.ds(at, span)] = flipped
        highs = []
        lows = []
        for c in range(3):
            load = jnp.sum(picked[c * nz : (c + 1) * nz] * flipped, axis=0, keepdims=True)
            high = load.astype(BF16).astype(F32)
            highs.append(high)
            lows.append(load - high)
        loads[:, pl.ds(at, span)] = jnp.concatenate(
            highs + lows + [jnp.zeros((2, span), F32)], axis=0
        )
        return carry

    lax.fori_loop(0, steps, load_step, 0)
    chains = [None, None]
    for k in range(steps):
        at = k * span
        value = loads[:, at : at + span]
        value = jnp.concatenate([value, value], axis=0).astype(BF16)
        value = jnp.concatenate([value] * (devices // 2), axis=0)
        spread = jnp.where(
            owner_mask(devices, own[:, at : at + span]), value, jnp.zeros(value.shape, BF16)
        )
        for number in range(2):
            band = slice(number * devices * 4, (number + 1) * devices * 4)
            add_to(chains, number, dot_nt(spread[band], slot_hot[:, at : at + span]))
    routed = jnp.concatenate(chains, axis=0)
    for o in range(devices):
        tile = routed[o * 8 : o * 8 + 3] + routed[o * 8 + 3 : o * 8 + 6]
        pay[o] = jnp.concatenate(
            [tile[:, p * LANES : (p + 1) * LANES] for p in range(parts)], axis=0
        )
    batch = math.gcd(devices, 8)
    send_all(
        grid, lambda o: pay.at[o], lambda m: pay_in.at[m], pay_send.at[0],
        lambda j: pay_recv.at[lax.div(j, batch)],
    )
    pay_in[me] = pay[me]

    settle(grid, node_in.at[others], node_sem.at[0], node_sem.at[1])

    def hot_step(d, carry):
        _, col = node_parts(node_in[d], rows, cols)
        node_hot[d] = one_hot(2 * cols, col)
        return carry

    lax.fori_loop(0, devices, hot_step, 0, unroll=4)

    def collide_step(row, carry):
        collide_row(pop, mom, read, yu_out, yd_out, row)
        return carry

    lax.fori_loop(0, nx, collide_step, 0, unroll=2)
    lb_copies = []

    def lb_copy(number, dx, dy, source, target):
        lb_copies.append(
            neighbour_copy(grid, dx, dy, source, target, lb_send.at[number], lb_recv.at[number])
        )

    for k, q in enumerate(x_up):
        lb_copy(0, 1, 0, read.at[q, 0], xu_in.at[k])
    for k, q in enumerate(x_down):
        lb_copy(1, -1, 0, read.at[q, nx - 1], xd_in.at[k])
    for k, q in enumerate(diagonal):
        dx, dy, _ = lattice_dirs[q]
        edge = yu_out.at[y_up.index(q)] if dy == 1 else yd_out.at[y_down.index(q)]
        lb_copy(2, dx, dy, edge.at[0 if dx == 1 else nx - 1], corner_in.at[k])
    lb_copy(3, 0, 1, yu_out, yu_in)
    lb_copy(4, 0, -1, yd_out, yd_in)

    def pay_arrived(step):
        got = batch - 1 if step == 0 else batch
        settle(grid, pay_in.at[pl.ds(0, got)], None, pay_recv.at[step])

    gather_force(grid, parts, node_in, node_hot, pay_in, force, pay_arrived)
    pack_side(force, side_out)
    for copy in rim_copies(grid, force, side_out, strip, rim_sem.at[0], rim_sem.at[1]) + lb_copies:
        copy.start()

    def sender(back, back_in, sem):
        def ready(j):
            @pl.when(j < devices)
            def _():
                other = lax.rem(me + devices - j, devices)
                pltpu.make_async_remote_copy(
                    src_ref=back.at[other],
                    dst_ref=back_in.at[me],
                    send_sem=sem.at[0],
                    recv_sem=sem.at[1],
                    device_id=(lax.div(other, grid[1]), lax.rem(other, grid[1])),
                    device_id_type=MESH,
                ).start()

        return ready

    pick_nodes(
        grid, parts, [force[c] for c in range(3)], node_in, node_hot, back_f,
        sender(back_f, back_f_in, backf_sem),
    )
    back_f_in[me] = back_f[me]

    def back_row(a):
        return pltpu.roll(a, full[0] - 1, 0)

    def back_col(a):
        return pltpu.roll(a, full[1] - 1, 1)

    settle(grid, stat_strip, stat_sem.at[0], stat_sem.at[1])
    moduli = with_rim(stat, stat_strip, 0)
    live = with_rim(stat, stat_strip, 1)
    mass = with_rim(stat, stat_strip, 2)
    next_row = back_row(moduli)
    scale = live * (moduli + next_row + back_col(moduli) + back_col(next_row)) * 0.25

    def operate(fields):
        down = [back_row(f) for f in fields]
        corners = (
            list(fields) + down + [back_col(f) for f in fields] + [back_col(f) for f in down]
        )
        results = []
        for k in range(12):
            total = stiff[k, 0] * corners[0]
            for l in range(1, 12):
                total = total + stiff[k, l] * corners[l]
            results.append(scale * total)
        images = []
        for c in range(3):
            right = results[6 + c] + pltpu.roll(results[9 + c], 1, 0)
            images.append(
                mass * fields[c]
                + results[c]
                + pltpu.roll(results[3 + c], 1, 0)
                + pltpu.roll(right, 1, 1)
            )
        return images

    def inner(a, b):
        total = a[0] * b[0]
        for c in range(1, 3):
            total = total + a[c] * b[c]
        return jnp.sum(jnp.sum(total, axis=0, keepdims=True), axis=1, keepdims=True)

    settle(grid, strip, rim_sem.at[0], rim_sem.at[1])
    field = [with_rim(force, strip, c) for c in range(3)]
    image = operate(field)
    f = [a[:rows, :cols] for a in field]
    q = [a[:rows, :cols] for a in image]
    for c in range(3):
        image_buf[c] = q[c]
    pick_nodes(grid, parts, q, node_in, node_hot, back_q, sender(back_q, back_q_in, backq_sem))
    back_q_in[me] = back_q[me]
    second = operate(image)
    s = [a[:rows, :cols] for a in second]
    ff, fq, qq, qs = inner(f, f), inner(f, q), inner(q, q), inner(q, s)
    guess = jnp.where(qq > 0.0, fq / jnp.where(qq > 0.0, qq, 1.0), 0.0)
    r0 = [f[c] - guess * q[c] for c in range(3)]
    u0 = [q[c] - guess * s[c] for c in range(3)]
    mine = [
        ff, fq, qq, qs, guess, inner(r0, r0), inner(r0, q), inner(r0, u0), inner(r0, s), inner(q, u0)
    ]
    lane = iota((1, LANES), 1)
    line = jnp.zeros((1, LANES), F32)
    for k, value in enumerate(mine):
        line = jnp.where(lane == k, value, line)
    sums[me] = line
    send_all(
        grid, lambda o: sums.at[me], lambda m: sums.at[m], sum_sem.at[0], lambda j: sum_sem.at[1]
    )

    settle(grid, xu_in, lb_send.at[0], lb_recv.at[0])
    settle(grid, xd_in, lb_send.at[1], lb_recv.at[1])
    settle(grid, corner_in, lb_send.at[2], lb_recv.at[2])
    settle(grid, yu_in, lb_send.at[3], lb_recv.at[3])
    settle(grid, yd_in, lb_send.at[4], lb_recv.at[4])
    mend_edges(read, xu_in, xd_in, yu_in, yd_in, corner_in)
    for k in range(steps):
        hot = one_hot(blocks, blk[:, k * span : (k + 1) * span])
        hot_turned[k * span : (k + 1) * span] = hot.T
    settle(grid, sums.at[others], sum_sem.at[0], sum_sem.at[1])
    every = sums[...].reshape(devices, LANES)
    ff, fq, qq, qs, guess, r0r0, r0q, r0u0, r0s, qu0 = [
        every[:, k : k + 1] for k in range(len(mine))
    ]

    def total(value):
        return jnp.sum(value, axis=0, keepdims=True)

    ff_all, fq_all = total(ff), total(fq)
    first = ff_all / fq_all
    off = guess - first
    rr = total(r0r0 + off * (2.0 * r0q + off * qq))
    rs = total(r0u0 + off * (r0s + qu0 + off * qs))
    rq = total(r0q + off * qq)
    ratio = rr / ff_all
    step_two = rr / (rs + 2.0 * ratio * rq + ratio * ratio * fq_all)
    alpha = first + step_two * (1.0 + ratio)
    beta = -(step_two * first)
    scal_out[0:1] = jnp.broadcast_to(alpha, (1, LANES))
    scal_out[1:2] = jnp.broadcast_to(beta, (1, LANES))
    settle(grid, pay.at[others], pay_send.at[0], None)
    settle(grid, back_f_in.at[others], backf_sem.at[0], backf_sem.at[1])
    settle(grid, back_q_in.at[others], backq_sem.at[0], backq_sem.at[1])


def couple(grid, parts, stiff, populations, weights, blk, own, node, modulus, live, mass):
    devices = grid[0] * grid[1]
    _, nx, ny, nz = populations.shape
    records = weights.shape[0]
    patch = (3,) + mass.shape
    slots = parts * LANES
    vmem = pl.BlockSpec(memory_space=pltpu.VMEM)
    hbm = pl.BlockSpec(memory_space=pltpu.HBM)
    rim = [pltpu.VMEM((2, 3, 8, patch[2]), F32), pltpu.VMEM((8, 3, 8, patch[2]), F32)]
    pay = (devices, 3 * parts, LANES)
    back = jax.ShapeDtypeStruct(pay, F32)
    dma = pltpu.SemaphoreType.DMA
    lines = pltpu.VMEM((1, records), jnp.int32)
    edges = pltpu.VMEM((5, nx, 1, nz), F32)
    return pl.pallas_call(
        functools.partial(couple_kernel, grid, parts),
        in_specs=[hbm] * 9,
        out_specs=[vmem] * 10,
        out_shape=[
            jax.ShapeDtypeStruct(populations.shape, F32),
            jax.ShapeDtypeStruct((nz, records), F32),
            jax.ShapeDtypeStruct(patch, F32),
            jax.ShapeDtypeStruct(patch, F32),
            jax.ShapeDtypeStruct((slots, records), BF16),
            jax.ShapeDtypeStruct((records, nx * ny), BF16),
            jax.ShapeDtypeStruct((2, LANES), F32),
            back,
            back,
            jax.ShapeDtypeStruct((1, records), jnp.int32),
        ],
        scratch_shapes=[
            pltpu.SMEM(stiff.shape, F32),
            pltpu.VMEM(populations.shape, F32),
            pltpu.VMEM((3, nx, ny, nz), F32),
            pltpu.VMEM((3 * nz, 2 * nx * ny), BF16),
            pltpu.VMEM(weights.shape, F32),
            lines, lines,
            pltpu.VMEM((8, records), F32),
            pltpu.VMEM((5, ny, nz), F32),
            pltpu.VMEM((5, ny, nz), F32),
            edges, edges, edges, edges,
            pltpu.VMEM((4, 1, nz), F32),
            pltpu.VMEM((devices, 1, slots), F32),
            pltpu.VMEM((devices, 1, slots), F32),
            pltpu.VMEM((devices, 2 * patch[2], slots), BF16),
            pltpu.VMEM(pay, F32),
            pltpu.VMEM(pay, F32),
            pltpu.VMEM(pay, F32),
            pltpu.VMEM(pay, F32),
            pltpu.VMEM(mass.shape, jnp.int32),
            pltpu.VMEM(patch, F32),
            *rim,
            *rim,
            pltpu.VMEM((devices, 1, LANES), F32),
            dma((4,)), dma((records // (4 * LANES),)), dma((7,)),
            dma((2,)), dma((1,)), dma((devices // math.gcd(devices, 8),)), dma((2,)), dma((2,)),
            dma((5,)), dma((5,)), dma((2,)), dma((2,)), dma((2,)),
        ],
        compiler_params=pltpu.CompilerParams(
            collective_id=0, has_side_effects=True, vmem_limit_bytes=36 * 2**20
        ),
        name="couple",
    )(stiff, populations, weights, blk, own, node, modulus, live, mass)


def finish_kernel(
    parts, scal, force, image, backf, backq, own, slot_hot, hot_turned, turned, read,
    out_hbm, disp_hbm,
    out, forcing, moved, disp, out_sem,
):
    devices = backf.shape[0]
    depth, records = turned.shape
    _, nx, ny, nz = read.shape
    blocks = nx * ny
    slots = parts * LANES
    span = 4 * LANES
    steps = records // span
    stages = [
        [q for q in range(1, 19) if lattice_dirs[q][1] == 0 and lattice_dirs[q][2] == 0],
        [q for q in range(19) if lattice_dirs[q][1] != 0 and lattice_dirs[q][2] == 0],
        [q for q in range(19) if lattice_dirs[q][2] != 0],
    ]
    out_copies = [
        pltpu.make_async_copy(out.at[q], out_hbm.at[q], out_sem.at[q]) for q in range(19)
    ]
    alpha = scal[0:1]
    beta = scal[1:2]

    def rest_step(row, carry):
        out[0, row] = read[0, row]
        return carry

    lax.fori_loop(0, nx, rest_step, 0, unroll=4)
    out_copies[0].start()
    for c in range(3):
        disp[c] = alpha * force[c] + beta * image[c]
    disp_copy = pltpu.make_async_copy(disp, disp_hbm, out_sem.at[19])
    disp_copy.start()
    back = alpha.reshape(1, 1, LANES) * backf[...] + beta.reshape(1, 1, LANES) * backq[...]
    wide = jnp.concatenate([back[:, p * 3 : p * 3 + 3] for p in range(parts)], axis=2)
    high = wide.astype(BF16).astype(F32)
    left = jnp.concatenate([high, wide - high, jnp.zeros((devices, 2, slots), F32)], axis=1)
    left = left.reshape(devices * 8, slots).astype(BF16)

    def move_step(k, carry):
        at = pl.multiple_of(k * span, span)
        found = dot_nn(left, slot_hot[:, pl.ds(at, span)])
        owners = own[:, pl.ds(at, span)]
        lines = [jnp.zeros((8, span), F32) for _ in range(4)]
        for o in range(devices):
            lines[o % 4] = lines[o % 4] + jnp.where(owners == o, found[o * 8 : o * 8 + 8], 0.0)
        lines = (lines[0] + lines[1]) + (lines[2] + lines[3])
        value = coupling * (lines[:3] + lines[3:6])
        moved[:, pl.ds(at, span)] = jnp.concatenate([value, jnp.zeros((5, span), F32)], axis=0)
        return carry

    lax.fori_loop(0, steps, move_step, 0, unroll=2)
    for c in range(3):
        chains = [None, None]
        for k in range(steps):
            at = k * span
            high, low = halves(turned[:, at : at + span] * moved[c : c + 1, at : at + span])
            for number in range(2):
                band = slice(number * depth // 2, (number + 1) * depth // 2)
                left = jnp.concatenate([high[band], low[band]], axis=0)
                add_to(chains, number, dot_nn(left, hot_turned[at : at + span]))
        chains = [chain[: depth // 2] + chain[depth // 2 :] for chain in chains]
        forcing[c] = jnp.concatenate(chains, axis=0).T.reshape(nx, ny, nz)

        def row_step(row, carry, c=c):
            fields = [forcing[axis_pos, row] if axis_pos <= c else None for axis_pos in range(3)]
            for q in stages[c]:
                projected = combine_dirs(fields, lattice_dirs[q])
                out[q, row] = read[q, row] + (3.0 * lattice_weights[q]) * projected
            return carry

        lax.fori_loop(0, nx, row_step, 0, unroll=2)
        for q in stages[c]:
            out_copies[q].start()
    disp_copy.wait()
    for copy in out_copies:
        copy.wait()


def finish(parts, scal, force, image, back_f, back_q, own, slot_hot, hot_turned, turned, read):
    hbm = pl.BlockSpec(memory_space=pltpu.HBM)
    vmem = pl.BlockSpec(memory_space=pltpu.VMEM)
    records = own.shape[1]
    dma = pltpu.SemaphoreType.DMA
    return pl.pallas_call(
        functools.partial(finish_kernel, parts),
        in_specs=[vmem] * 10,
        out_specs=[hbm, hbm],
        out_shape=[
            jax.ShapeDtypeStruct(read.shape, F32),
            jax.ShapeDtypeStruct(force.shape, F32),
        ],
        scratch_shapes=[
            pltpu.VMEM(read.shape, F32),
            pltpu.VMEM((3,) + read.shape[1:], F32),
            pltpu.VMEM((8, records), F32),
            pltpu.VMEM(force.shape, F32),
            dma((20,)),
        ],
        compiler_params=pltpu.CompilerParams(vmem_limit_bytes=24 * 2**20),
        name="finish",
    )(scal, force, image, back_f, back_q, own, slot_hot, hot_turned, turned, read)


def per_device(
    grid, populations, mass, modulus, cell_live, stiff_ref, rec_block, rec_owner, rec_node,
    rbf_weight,
):
    devices = grid[0] * grid[1]
    records = rec_block.shape[0]
    capacity = 2 * records // devices
    parts = -(-capacity // LANES)
    blk = rec_block.reshape(1, records)
    own = rec_owner.reshape(1, records)
    node = rec_node.reshape(1, records)
    operands = [
        pltpu.with_memory_space_constraint(a, pltpu.HBM)
        for a in (stiff_ref, populations, rbf_weight, blk, own, node, modulus, cell_live, mass)
    ]
    read, turned, force, image, slot_hot, hot_turned, scal, back_f, back_q, held_own = couple(
        grid, parts, *operands
    )
    return finish(
        parts, scal, force, image, back_f, back_q, held_own, slot_hot, hot_turned, turned, read
    )


def solution(mesh):
    grid = (mesh.shape["gx"], mesh.shape["gy"])
    in_specs = (
        P(None, "gx", "gy", None),
        P("gx", "gy"),
        P("gx", "gy"),
        P("gx", "gy"),
        P(),
        P(("gx", "gy")),
        P(("gx", "gy"), None),
        P(("gx", "gy")),
        P(("gx", "gy"), None),
    )
    out_specs = (P(None, "gx", "gy", None), P(None, "gx", "gy"))
    return jax.shard_map(
        functools.partial(per_device, grid), mesh=mesh, in_specs=in_specs, out_specs=out_specs,
        check_vma=False,
    )
```

```python
import functools
import math

import jax
import jax.numpy as jnp
from jax import lax
from jax.experimental import pallas as pl
from jax.experimental.pallas import tpu as pltpu
from jax.sharding import PartitionSpec as P

MESH = pl.DeviceIdType.MESH
F32 = jnp.float32
BF16 = jnp.bfloat16
LANES = 128

lattice_dirs = (
    (0, 0, 0),
    (1, 0, 0),
    (-1, 0, 0),
    (0, 1, 0),
    (0, -1, 0),
    (0, 0, 1),
    (0, 0, -1),
    (1, 1, 0),
    (-1, -1, 0),
    (1, -1, 0),
    (-1, 1, 0),
    (1, 0, 1),
    (-1, 0, -1),
    (1, 0, -1),
    (-1, 0, 1),
    (0, 1, 1),
    (0, -1, -1),
    (0, 1, -1),
    (0, -1, 1),
)
lattice_weights = (1.0 / 3.0,) + (1.0 / 18.0,) * 6 + (1.0 / 36.0,) * 12
relax_rate = 1.25
coupling = 0.1

x_up = [q for q in range(19) if lattice_dirs[q][0] == 1]
x_down = [q for q in range(19) if lattice_dirs[q][0] == -1]
y_up = [q for q in range(19) if lattice_dirs[q][1] == 1]
y_down = [q for q in range(19) if lattice_dirs[q][1] == -1]
diagonal = [q for q in range(19) if lattice_dirs[q][0] != 0 and lattice_dirs[q][1] != 0]


def combine_dirs(fields, direction):
    total = None
    for axis_pos in range(3):
        if direction[axis_pos] != 0:
            field = fields[axis_pos]
            if total is None:
                total = field if direction[axis_pos] == 1 else -field
            else:
                total = total + field if direction[axis_pos] == 1 else total - field
    return total


def halves(values):
    high = values.astype(BF16)
    low = (values - high.astype(F32)).astype(BF16)
    return high, low


def iota(shape, dim):
    return lax.broadcasted_iota(jnp.int32, shape, dim)


def dot_nt(left, right):
    return lax.dot_general(left, right, (((1,), (1,)), ((), ())), preferred_element_type=F32)


def dot_nn(left, right):
    return lax.dot_general(left, right, (((1,), (0,)), ((), ())), preferred_element_type=F32)


def position(grid):
    return lax.axis_index("gx"), lax.axis_index("gy")


def each_other(devices, body):
    batch = 6
    rounds = (devices - 1) // batch

    def one(step, carry):
        for d in range(batch):
            body(step * batch + d + 1)
        return carry

    lax.fori_loop(0, rounds, one, 0)
    for j in range(rounds * batch + 1, devices):
        body(j)


def greet_all(grid):
    ix, iy = position(grid)
    devices = grid[0] * grid[1]
    me = ix * grid[1] + iy
    barrier = pltpu.get_barrier_semaphore()

    def signal(j):
        other = lax.rem(me + j, devices)
        pl.semaphore_signal(
            barrier, inc=1, device_id=(lax.div(other, grid[1]), lax.rem(other, grid[1])),
            device_id_type=MESH,
        )

    each_other(devices, signal)


def await_all(grid):
    pl.semaphore_wait(pltpu.get_barrier_semaphore(), grid[0] * grid[1] - 1)


def send_all(grid, source, target, send_sem, recv_sem):
    ix, iy = position(grid)
    devices = grid[0] * grid[1]
    me = ix * grid[1] + iy

    def body(j):
        other = lax.rem(me + j, devices)
        pltpu.make_async_remote_copy(
            src_ref=source(other),
            dst_ref=target(me),
            send_sem=send_sem,
            recv_sem=recv_sem(j),
            device_id=(lax.div(other, grid[1]), lax.rem(other, grid[1])),
            device_id_type=MESH,
        ).start()

    each_other(devices, body)


def neighbour_copy(grid, dx, dy, source, target, send_sem, recv_sem):
    ix, iy = position(grid)
    return pltpu.make_async_remote_copy(
        src_ref=source,
        dst_ref=target,
        send_sem=send_sem,
        recv_sem=recv_sem,
        device_id=(lax.rem(ix + dx + grid[0], grid[0]), lax.rem(iy + dy + grid[1], grid[1])),
        device_id_type=MESH,
    )


def pack_side(field, side_out):
    rows, cols = field.shape[1:]
    for c in range(3):
        tall = jnp.concatenate([field[c], jnp.zeros((cols - rows, cols), F32)], axis=0).T
        side_out[0, c] = tall[cols - 8 :]
        side_out[1, c] = tall[:8]


def rim_copies(grid, field, side_out, strip, send_sem, recv_sem):
    rows = field.shape[1]
    copies = []
    for k in range(3):
        dy = 1 - k
        copies.append(
            neighbour_copy(
                grid, 1, dy, field.at[:, pl.ds(rows - 8, 8), :], strip.at[k], send_sem, recv_sem
            )
        )
        copies.append(
            neighbour_copy(
                grid, -1, dy, field.at[:, pl.ds(0, 8), :], strip.at[3 + k], send_sem, recv_sem
            )
        )
    copies.append(neighbour_copy(grid, 0, 1, side_out.at[0], strip.at[6], send_sem, recv_sem))
    copies.append(neighbour_copy(grid, 0, -1, side_out.at[1], strip.at[7], send_sem, recv_sem))
    return copies


def settle(grid, buffer, send_sem, recv_sem):
    copy = neighbour_copy(
        grid, 0, 1, buffer, buffer, recv_sem if send_sem is None else send_sem,
        send_sem if recv_sem is None else recv_sem,
    )
    if send_sem is not None:
        copy.wait_send()
    if recv_sem is not None:
        copy.wait_recv()


def with_rim(centre, strip, c):
    rows, cols = centre.shape[1:]
    beside = jnp.concatenate([strip[7, c], jnp.zeros((cols - 16, cols), F32), strip[6, c]], axis=0)
    main = jnp.concatenate([centre[c], beside.T[:rows]], axis=1)
    low = iota((8, cols), 0) < 4
    left_strip = iota((8, cols), 1) < cols // 2
    below = jnp.where(low, strip[4, c], strip[1, c])
    corner = jnp.where(
        low,
        jnp.where(left_strip, strip[5, c], strip[3, c]),
        jnp.where(left_strip, strip[2, c], strip[0, c]),
    )
    return jnp.concatenate([main, jnp.concatenate([below, corner], axis=1)], axis=0)


def spread_rows(values, count):
    rows = jnp.broadcast_to(values, (16, values.shape[1])).astype(BF16)
    return jnp.concatenate([rows] * (count // 16), axis=0)


def one_hot(count, index):
    index = index.astype(F32)
    ramp = iota((count, index.shape[1]), 0).astype(F32).astype(BF16)
    one = jnp.ones(ramp.shape, BF16)
    return jnp.where(ramp == spread_rows(index, count), one, jnp.zeros(ramp.shape, BF16))


def add_to(chains, number, part):
    held = chains[number]
    chains[number] = part if held is None else held + part


def owner_mask(devices, owners):
    lines = (iota((devices * 8, owners.shape[1]), 0) // 8).astype(F32).astype(BF16)
    return lines == spread_rows(owners.astype(F32), devices * 8)


def find_slots(devices, node_cols, own_ref, node_ref, slot_hot, node_pay):
    records = own_ref.shape[1]
    slots = slot_hot.shape[0]
    span = 2 * LANES
    steps = records // span
    before = (iota((span, span), 0) <= iota((span, span), 1)).astype(F32).astype(BF16)
    base = jnp.full((devices, span), -1.0, F32)
    routed = None
    for i in range(steps):
        hits = one_hot(devices, own_ref[:, i * span : (i + 1) * span])
        counts = dot_nn(hits, before)
        slot = jnp.sum(hits.astype(F32) * (counts + base), axis=0, keepdims=True)
        base = base + jnp.broadcast_to(counts[:, span - 1 :], (devices, span))
        hot = one_hot(slots, slot)
        slot_hot[:, i * span : (i + 1) * span] = hot
        node = node_ref[:, i * span : (i + 1) * span]
        row = node // node_cols
        col = node - row * node_cols
        left = jnp.concatenate(
            [
                hits * spread_rows(row.astype(F32), devices),
                hits * spread_rows(col.astype(F32), devices),
            ],
            axis=0,
        )
        part = dot_nt(left, hot)
        routed = part if routed is None else routed + part
    nodes = routed[:devices] * float(node_cols) + routed[devices:]
    for o in range(devices):
        node_pay[o] = nodes[o : o + 1]


def moments(pop, mom, row):
    for axis_pos in range(3):
        total = None
        for q in range(19):
            sign = lattice_dirs[q][axis_pos]
            if sign == 1:
                total = pop[q, row] if total is None else total + pop[q, row]
            elif sign == -1:
                total = -pop[q, row] if total is None else total - pop[q, row]
        mom[axis_pos, row] = total


def collide_row(pop, mom, read, yu, yd, row):
    rows, cols, depth = read.shape[1:]
    pops = [pop[q, row] for q in range(19)]
    density = pops[0]
    for q in range(1, 19):
        density = density + pops[q]
    inverse = 1.0 / density
    velocity = [mom[axis_pos, row] * inverse for axis_pos in range(3)]
    squared = velocity[0] * velocity[0] + velocity[1] * velocity[1] + velocity[2] * velocity[2]
    rest = 1.0 - 1.5 * squared
    scaled = {w: (relax_rate * w) * density for w in sorted(set(lattice_weights))}
    ups = lax.rem(row + 1, rows)
    downs = lax.rem(row + rows - 1, rows)
    for q in range(19):
        dx, dy, dz = lattice_dirs[q]
        projected = combine_dirs(velocity, lattice_dirs[q])
        bracket = rest
        if projected is not None:
            bracket = rest + projected * (3.0 + 4.5 * projected)
        value = (1.0 - relax_rate) * pops[q] + scaled[lattice_weights[q]] * bracket
        if dz != 0:
            value = pltpu.roll(value, dz % depth, 1)
        if dy != 0:
            value = pltpu.roll(value, dy % cols, 0)
        at = ups if dx == 1 else downs if dx == -1 else row
        read[q, at] = value
        if dy == 1:
            yu[y_up.index(q), at] = value[0:1]
        if dy == -1:
            yd[y_down.index(q), at] = value[cols - 1 : cols]


def mend_edges(read, xu, xd, yu, yd, corner):
    rows, cols, depth = read.shape[1:]
    for k, q in enumerate(x_up):
        read[q, 0] = xu[k]
    for k, q in enumerate(x_down):
        read[q, rows - 1] = xd[k]

    def one(row, carry):
        for k, q in enumerate(y_up):
            read[q, row, 0:1] = yu[k, row]
        for k, q in enumerate(y_down):
            read[q, row, cols - 1 : cols] = yd[k, row]
        return carry

    lax.fori_loop(0, rows, one, 0, unroll=4)
    for k, q in enumerate(diagonal):
        dx, dy, _ = lattice_dirs[q]
        at = 0 if dy == 1 else cols - 1
        read[q, 0 if dx == 1 else rows - 1, at : at + 1] = corner[k]


def sources_of(grid, step, count):
    ix, iy = position(grid)
    devices = grid[0] * grid[1]
    me = ix * grid[1] + iy
    return [
        lax.rem(me + devices - lax.rem(step * count + d + 1, devices), devices)
        for d in range(count)
    ]


def node_parts(node, rows, cols):
    node = node.astype(jnp.int32)
    half = rows // 2 * cols
    top = node // half
    rest = node - top * half
    row = rest // cols
    return row, rest - row * cols + top * cols


def lane_row(ref, source, c, parts):
    return jnp.concatenate(
        [ref[source, p * 3 + c : p * 3 + c + 1] for p in range(parts)], axis=1
    )


def gather_force(grid, parts, node_in, node_hot, pay, force, arrived):
    ix, iy = position(grid)
    devices = pay.shape[0]
    me = ix * grid[1] + iy
    rows, cols = force.shape[1:]
    half = rows // 2
    count = math.gcd(devices, 8)
    chains = [None, None]
    for step in range(devices // count):
        arrived(step)
        for d in range(count):
            source = lax.rem(me + devices - (step * count + d), devices)
            row, _ = node_parts(node_in[source], rows, cols)
            row_hot = one_hot(half, row)
            highs = []
            lows = []
            for c in range(3):
                value = lane_row(pay, source, c, parts)
                high = value.astype(BF16).astype(F32)
                highs.append(row_hot * spread_rows(high, half))
                lows.append(row_hot * spread_rows(value - high, half))
            for number in range(2):
                lines = slice(number * half // 2, (number + 1) * half // 2)
                left = jnp.concatenate([piece[lines] for piece in highs + lows], axis=0)
                add_to(chains, number, dot_nt(left, node_hot[source]))
    middle = half // 2
    chains = [chain[: 3 * middle] + chain[3 * middle :] for chain in chains]
    for c in range(3):
        piece = jnp.concatenate(
            [chain[c * middle : (c + 1) * middle] for chain in chains], axis=0
        )
        force[c] = jnp.concatenate([piece[:, :cols], piece[:, cols:]], axis=0)


def pick_nodes(grid, parts, field, node_in, node_hot, out, ready):
    devices = out.shape[0]
    rows, cols = field[0].shape
    half = rows // 2
    slots = parts * LANES
    count = math.gcd(devices, 8)
    wide = [jnp.concatenate([f[:half], f[half:]], axis=1) for f in field]
    high, low = halves(jnp.concatenate(wide, axis=0))
    left = jnp.concatenate([high, low], axis=0)

    def one(step, carry):
        sources = sources_of(grid, step, count)
        for source in sources:
            row, _ = node_parts(node_in[source], rows, cols)
            row_hot = iota((half, slots), 0) == row
            found = dot_nn(left, node_hot[source])
            found = found[: 3 * half] + found[3 * half :]
            values = [
                jnp.sum(
                    jnp.where(row_hot, found[c * half : (c + 1) * half], 0.0), axis=0, keepdims=True
                )
                for c in range(3)
            ]
            out[source] = jnp.concatenate(
                [value[:, p * LANES : (p + 1) * LANES] for p in range(parts) for value in values],
                axis=0,
            )
        for d in range(count):
            ready(step * count + d + 1)
        return carry

    lax.fori_loop(0, devices // count, one, 0)


def couple_kernel(
    grid, parts, stiff_hbm, pop_hbm, w_hbm, blk_hbm, own_hbm, node_hbm, modulus_hbm, live_hbm, mass_hbm,
    read, turned, force, image_buf, slot_hot, hot_turned, scal_out, back_f_in, back_q_in, own,
    stiff, pop, mom, mom_cat, w, node, blk, loads,
    xu_in, xd_in, yu_out, yd_out, yu_in, yd_in, corner_in,
    node_pay, node_in, node_hot, pay, pay_in, back_f, back_q,
    live_in, stat, stat_out, stat_strip, side_out, strip, sums,
    pop_sem, w_sem, small_sem,
    node_sem, pay_send, pay_recv, backf_sem, backq_sem, lb_send, lb_recv, stat_sem, rim_sem, sum_sem,
):
    ix, iy = position(grid)
    devices = grid[0] * grid[1]
    me = ix * grid[1] + iy
    rows, cols = force.shape[1:]
    full = (rows + 8, 2 * cols)
    nx, ny, nz = read.shape[1:]
    blocks = nx * ny
    records = w.shape[0]
    slots = parts * LANES
    others = pl.ds(0, devices - 1)
    greet_all(grid)
    small = [
        pltpu.make_async_copy(source, target, small_sem.at[k])
        for k, (source, target) in enumerate(
            [
                (own_hbm, own), (node_hbm, node), (blk_hbm, blk), (modulus_hbm, stat.at[0]),
                (mass_hbm, stat.at[2]), (live_hbm, live_in), (stiff_hbm, stiff),
            ]
        )
    ]
    pop_rows = nx // 4
    pop_copies = [
        pltpu.make_async_copy(
            pop_hbm.at[:, pl.ds(k * pop_rows, pop_rows)], pop.at[:, pl.ds(k * pop_rows, pop_rows)],
            pop_sem.at[k],
        )
        for k in range(4)
    ]
    span = 4 * LANES
    steps = records // span

    def w_copy(k):
        at = pl.multiple_of(k * span, span)
        return pltpu.make_async_copy(w_hbm.at[pl.ds(at, span)], w.at[pl.ds(at, span)], w_sem.at[k])

    for copy in small + pop_copies:
        copy.start()
    for copy in small[:3]:
        copy.wait()
    find_slots(devices, cols, own, node, slot_hot, node_pay)

    for k, copy in enumerate(pop_copies):
        copy.wait()
        if k == 1:
            for number in range(steps):
                w_copy(number).start()

        def moment_row(row, carry):
            moments(pop, mom, row)
            return carry

        lax.fori_loop(k * pop_rows, (k + 1) * pop_rows, moment_row, 0, unroll=2)
    for c in range(3):
        high, low = halves(mom[c].reshape(blocks, nz).T)
        mom_cat[c * nz : (c + 1) * nz, :blocks] = high
        mom_cat[c * nz : (c + 1) * nz, blocks:] = low
    for copy in small[3:]:
        copy.wait()
    stat[1] = live_in[...].astype(F32)
    pack_side(stat, stat_out)
    await_all(grid)
    send_all(
        grid, lambda o: node_pay.at[o], lambda m: node_in.at[m], node_sem.at[0],
        lambda j: node_sem.at[1],
    )
    node_in[me] = node_pay[me]
    for copy in rim_copies(grid, stat, stat_out, stat_strip, stat_sem.at[0], stat_sem.at[1]):
        copy.start()

    def load_step(k, carry):
        w_copy(k).wait()
        at = pl.multiple_of(k * span, span)
        hot = one_hot(blocks, blk[:, pl.ds(at, span)])
        picked = dot_nn(mom_cat[...], jnp.concatenate([hot, hot], axis=0))
        flipped = w[pl.ds(at, span), :].T
        turned[:, pl.ds(at, span)] = flipped
        highs = []
        lows = []
        for c in range(3):
            load = jnp.sum(picked[c * nz : (c + 1) * nz] * flipped, axis=0, keepdims=True)
            high = load.astype(BF16).astype(F32)
            highs.append(high)
            lows.append(load - high)
        loads[:, pl.ds(at, span)] = jnp.concatenate(
            highs + lows + [jnp.zeros((2, span), F32)], axis=0
        )
        return carry

    lax.fori_loop(0, steps, load_step, 0)
    chains = [None, None]
    for k in range(steps):
        at = k * span
        value = loads[:, at : at + span]
        value = jnp.concatenate([value, value], axis=0).astype(BF16)
        value = jnp.concatenate([value] * (devices // 2), axis=0)
        spread = jnp.where(
            owner_mask(devices, own[:, at : at + span]), value, jnp.zeros(value.shape, BF16)
        )
        for number in range(2):
            band = slice(number * devices * 4, (number + 1) * devices * 4)
            add_to(chains, number, dot_nt(spread[band], slot_hot[:, at : at + span]))
    routed = jnp.concatenate(chains, axis=0)
    for o in range(devices):
        tile = routed[o * 8 : o * 8 + 3] + routed[o * 8 + 3 : o * 8 + 6]
        pay[o] = jnp.concatenate(
            [tile[:, p * LANES : (p + 1) * LANES] for p in range(parts)], axis=0
        )
    batch = math.gcd(devices, 8)
    send_all(
        grid, lambda o: pay.at[o], lambda m: pay_in.at[m], pay_send.at[0],
        lambda j: pay_recv.at[lax.div(j, batch)],
    )
    pay_in[me] = pay[me]

    settle(grid, node_in.at[others], node_sem.at[0], node_sem.at[1])

    def hot_step(d, carry):
        _, col = node_parts(node_in[d], rows, cols)
        node_hot[d] = one_hot(2 * cols, col)
        return carry

    lax.fori_loop(0, devices, hot_step, 0, unroll=4)

    def collide_step(row, carry):
        collide_row(pop, mom, read, yu_out, yd_out, row)
        return carry

    lax.fori_loop(0, nx, collide_step, 0, unroll=2)
    lb_copies = []

    def lb_copy(number, dx, dy, source, target):
        lb_copies.append(
            neighbour_copy(grid, dx, dy, source, target, lb_send.at[number], lb_recv.at[number])
        )

    for k, q in enumerate(x_up):
        lb_copy(0, 1, 0, read.at[q, 0], xu_in.at[k])
    for k, q in enumerate(x_down):
        lb_copy(1, -1, 0, read.at[q, nx - 1], xd_in.at[k])
    for k, q in enumerate(diagonal):
        dx, dy, _ = lattice_dirs[q]
        edge = yu_out.at[y_up.index(q)] if dy == 1 else yd_out.at[y_down.index(q)]
        lb_copy(2, dx, dy, edge.at[0 if dx == 1 else nx - 1], corner_in.at[k])
    lb_copy(3, 0, 1, yu_out, yu_in)
    lb_copy(4, 0, -1, yd_out, yd_in)

    def pay_arrived(step):
        got = batch - 1 if step == 0 else batch
        settle(grid, pay_in.at[pl.ds(0, got)], None, pay_recv.at[step])

    gather_force(grid, parts, node_in, node_hot, pay_in, force, pay_arrived)
    copies = rim_copies(grid, force, side_out, strip, rim_sem.at[0], rim_sem.at[1])
    for copy in copies[:6]:
        copy.start()
    pack_side(force, side_out)
    for copy in copies[6:] + lb_copies:
        copy.start()

    def sender(back, back_in, sem):
        def ready(j):
            @pl.when(j < devices)
            def _():
                other = lax.rem(me + devices - j, devices)
                pltpu.make_async_remote_copy(
                    src_ref=back.at[other],
                    dst_ref=back_in.at[me],
                    send_sem=sem.at[0],
                    recv_sem=sem.at[1],
                    device_id=(lax.div(other, grid[1]), lax.rem(other, grid[1])),
                    device_id_type=MESH,
                ).start()

        return ready

    pick_nodes(
        grid, parts, [force[c] for c in range(3)], node_in, node_hot, back_f,
        sender(back_f, back_f_in, backf_sem),
    )
    back_f_in[me] = back_f[me]

    def back_row(a):
        return pltpu.roll(a, full[0] - 1, 0)

    def back_col(a):
        return pltpu.roll(a, full[1] - 1, 1)

    settle(grid, stat_strip, stat_sem.at[0], stat_sem.at[1])
    moduli = with_rim(stat, stat_strip, 0)
    live = with_rim(stat, stat_strip, 1)
    mass = with_rim(stat, stat_strip, 2)
    next_row = back_row(moduli)
    scale = live * (moduli + next_row + back_col(moduli) + back_col(next_row)) * 0.25

    def operate(fields):
        down = [back_row(f) for f in fields]
        corners = (
            list(fields) + down + [back_col(f) for f in fields] + [back_col(f) for f in down]
        )
        results = []
        for k in range(12):
            total = stiff[k, 0] * corners[0]
            for l in range(1, 12):
                total = total + stiff[k, l] * corners[l]
            results.append(scale * total)
        images = []
        for c in range(3):
            right = results[6 + c] + pltpu.roll(results[9 + c], 1, 0)
            images.append(
                mass * fields[c]
                + results[c]
                + pltpu.roll(results[3 + c], 1, 0)
                + pltpu.roll(right, 1, 1)
            )
        return images

    def inner(a, b):
        total = a[0] * b[0]
        for c in range(1, 3):
            total = total + a[c] * b[c]
        return jnp.sum(jnp.sum(total, axis=0, keepdims=True), axis=1, keepdims=True)

    settle(grid, strip, rim_sem.at[0], rim_sem.at[1])
    field = [with_rim(force, strip, c) for c in range(3)]
    image = operate(field)
    f = [a[:rows, :cols] for a in field]
    q = [a[:rows, :cols] for a in image]
    for c in range(3):
        image_buf[c] = q[c]
    pick_nodes(grid, parts, q, node_in, node_hot, back_q, sender(back_q, back_q_in, backq_sem))
    back_q_in[me] = back_q[me]
    second = operate(image)
    s = [a[:rows, :cols] for a in second]
    ff, fq, qq, qs = inner(f, f), inner(f, q), inner(q, q), inner(q, s)
    guess = jnp.where(qq > 0.0, fq / jnp.where(qq > 0.0, qq, 1.0), 0.0)
    r0 = [f[c] - guess * q[c] for c in range(3)]
    u0 = [q[c] - guess * s[c] for c in range(3)]
    mine = [
        ff, fq, qq, qs, guess, inner(r0, r0), inner(r0, q), inner(r0, u0), inner(r0, s), inner(q, u0)
    ]
    lane = iota((1, LANES), 1)
    line = jnp.zeros((1, LANES), F32)
    for k, value in enumerate(mine):
        line = jnp.where(lane == k, value, line)
    sums[me] = line
    send_all(
        grid, lambda o: sums.at[me], lambda m: sums.at[m], sum_sem.at[0], lambda j: sum_sem.at[1]
    )

    settle(grid, xu_in, lb_send.at[0], lb_recv.at[0])
    settle(grid, xd_in, lb_send.at[1], lb_recv.at[1])
    settle(grid, corner_in, lb_send.at[2], lb_recv.at[2])
    settle(grid, yu_in, lb_send.at[3], lb_recv.at[3])
    settle(grid, yd_in, lb_send.at[4], lb_recv.at[4])
    mend_edges(read, xu_in, xd_in, yu_in, yd_in, corner_in)
    for k in range(steps):
        hot = one_hot(blocks, blk[:, k * span : (k + 1) * span])
        hot_turned[k * span : (k + 1) * span] = hot.T
    settle(grid, sums.at[others], sum_sem.at[0], sum_sem.at[1])
    every = sums[...].reshape(devices, LANES)
    ff, fq, qq, qs, guess, r0r0, r0q, r0u0, r0s, qu0 = [
        every[:, k : k + 1] for k in range(len(mine))
    ]

    def total(value):
        return jnp.sum(value, axis=0, keepdims=True)

    ff_all, fq_all = total(ff), total(fq)
    first = ff_all / fq_all
    off = guess - first
    rr = total(r0r0 + off * (2.0 * r0q + off * qq))
    rs = total(r0u0 + off * (r0s + qu0 + off * qs))
    rq = total(r0q + off * qq)
    ratio = rr / ff_all
    step_two = rr / (rs + 2.0 * ratio * rq + ratio * ratio * fq_all)
    alpha = first + step_two * (1.0 + ratio)
    beta = -(step_two * first)
    scal_out[0:1] = jnp.broadcast_to(alpha, (1, LANES))
    scal_out[1:2] = jnp.broadcast_to(beta, (1, LANES))
    settle(grid, pay.at[others], pay_send.at[0], None)
    settle(grid, back_f_in.at[others], backf_sem.at[0], backf_sem.at[1])
    settle(grid, back_q_in.at[others], backq_sem.at[0], backq_sem.at[1])


def couple(grid, parts, stiff, populations, weights, blk, own, node, modulus, live, mass):
    devices = grid[0] * grid[1]
    _, nx, ny, nz = populations.shape
    records = weights.shape[0]
    patch = (3,) + mass.shape
    slots = parts * LANES
    vmem = pl.BlockSpec(memory_space=pltpu.VMEM)
    hbm = pl.BlockSpec(memory_space=pltpu.HBM)
    rim = [pltpu.VMEM((2, 3, 8, patch[2]), F32), pltpu.VMEM((8, 3, 8, patch[2]), F32)]
    pay = (devices, 3 * parts, LANES)
    back = jax.ShapeDtypeStruct(pay, F32)
    dma = pltpu.SemaphoreType.DMA
    lines = pltpu.VMEM((1, records), jnp.int32)
    edges = pltpu.VMEM((5, nx, 1, nz), F32)
    return pl.pallas_call(
        functools.partial(couple_kernel, grid, parts),
        in_specs=[hbm] * 9,
        out_specs=[vmem] * 10,
        out_shape=[
            jax.ShapeDtypeStruct(populations.shape, F32),
            jax.ShapeDtypeStruct((nz, records), F32),
            jax.ShapeDtypeStruct(patch, F32),
            jax.ShapeDtypeStruct(patch, F32),
            jax.ShapeDtypeStruct((slots, records), BF16),
            jax.ShapeDtypeStruct((records, nx * ny), BF16),
            jax.ShapeDtypeStruct((2, LANES), F32),
            back,
            back,
            jax.ShapeDtypeStruct((1, records), jnp.int32),
        ],
        scratch_shapes=[
            pltpu.SMEM(stiff.shape, F32),
            pltpu.VMEM(populations.shape, F32),
            pltpu.VMEM((3, nx, ny, nz), F32),
            pltpu.VMEM((3 * nz, 2 * nx * ny), BF16),
            pltpu.VMEM(weights.shape, F32),
            lines, lines,
            pltpu.VMEM((8, records), F32),
            pltpu.VMEM((5, ny, nz), F32),
            pltpu.VMEM((5, ny, nz), F32),
            edges, edges, edges, edges,
            pltpu.VMEM((4, 1, nz), F32),
            pltpu.VMEM((devices, 1, slots), F32),
            pltpu.VMEM((devices, 1, slots), F32),
            pltpu.VMEM((devices, 2 * patch[2], slots), BF16),
            pltpu.VMEM(pay, F32),
            pltpu.VMEM(pay, F32),
            pltpu.VMEM(pay, F32),
            pltpu.VMEM(pay, F32),
            pltpu.VMEM(mass.shape, jnp.int32),
            pltpu.VMEM(patch, F32),
            *rim,
            *rim,
            pltpu.VMEM((devices, 1, LANES), F32),
            dma((4,)), dma((records // (4 * LANES),)), dma((7,)),
            dma((2,)), dma((1,)), dma((devices // math.gcd(devices, 8),)), dma((2,)), dma((2,)),
            dma((5,)), dma((5,)), dma((2,)), dma((2,)), dma((2,)),
        ],
        compiler_params=pltpu.CompilerParams(
            collective_id=0, has_side_effects=True, vmem_limit_bytes=36 * 2**20
        ),
        name="couple",
    )(stiff, populations, weights, blk, own, node, modulus, live, mass)


def finish_kernel(
    parts, scal, force, image, backf, backq, own, slot_hot, hot_turned, turned, read,
    out_hbm, disp_hbm,
    out, forcing, moved, disp, out_sem,
):
    devices = backf.shape[0]
    depth, records = turned.shape
    _, nx, ny, nz = read.shape
    blocks = nx * ny
    slots = parts * LANES
    span = 4 * LANES
    steps = records // span
    stages = [
        [q for q in range(1, 19) if lattice_dirs[q][1] == 0 and lattice_dirs[q][2] == 0],
        [q for q in range(19) if lattice_dirs[q][1] != 0 and lattice_dirs[q][2] == 0],
        [q for q in range(19) if lattice_dirs[q][2] != 0],
    ]
    out_copies = [
        pltpu.make_async_copy(out.at[q], out_hbm.at[q], out_sem.at[q]) for q in range(19)
    ]
    alpha = scal[0:1]
    beta = scal[1:2]

    def rest_step(row, carry):
        out[0, row] = read[0, row]
        return carry

    lax.fori_loop(0, nx, rest_step, 0, unroll=4)
    out_copies[0].start()
    for c in range(3):
        disp[c] = alpha * force[c] + beta * image[c]
    disp_copy = pltpu.make_async_copy(disp, disp_hbm, out_sem.at[19])
    disp_copy.start()
    back = alpha.reshape(1, 1, LANES) * backf[...] + beta.reshape(1, 1, LANES) * backq[...]
    wide = jnp.concatenate([back[:, p * 3 : p * 3 + 3] for p in range(parts)], axis=2)
    high = wide.astype(BF16).astype(F32)
    left = jnp.concatenate([high, wide - high, jnp.zeros((devices, 2, slots), F32)], axis=1)
    left = left.reshape(devices * 8, slots).astype(BF16)

    def move_step(k, carry):
        at = pl.multiple_of(k * span, span)
        found = dot_nn(left, slot_hot[:, pl.ds(at, span)])
        found = jnp.where(
            owner_mask(devices, own[:, pl.ds(at, span)]), found.astype(BF16),
            jnp.zeros(found.shape, BF16),
        )
        lines = found[:16]
        for o in range(1, devices // 2):
            lines = lines + found[o * 16 : (o + 1) * 16]
        lines = lines.astype(F32)
        lines = lines[:8] + lines[8:]
        value = coupling * (lines[:3] + lines[3:6])
        moved[:, pl.ds(at, span)] = jnp.concatenate([value, jnp.zeros((5, span), F32)], axis=0)
        return carry

    lax.fori_loop(0, steps, move_step, 0, unroll=2)
    for c in range(3):
        chains = [None, None]
        for k in range(steps):
            at = k * span
            high, low = halves(turned[:, at : at + span] * moved[c : c + 1, at : at + span])
            for number in range(2):
                band = slice(number * depth // 2, (number + 1) * depth // 2)
                left = jnp.concatenate([high[band], low[band]], axis=0)
                add_to(chains, number, dot_nn(left, hot_turned[at : at + span]))
        chains = [chain[: depth // 2] + chain[depth // 2 :] for chain in chains]
        forcing[c] = jnp.concatenate(chains, axis=0).T.reshape(nx, ny, nz)

        def row_step(row, carry, c=c):
            fields = [forcing[axis_pos, row] if axis_pos <= c else None for axis_pos in range(3)]
            for q in stages[c]:
                projected = combine_dirs(fields, lattice_dirs[q])
                out[q, row] = read[q, row] + (3.0 * lattice_weights[q]) * projected
            return carry

        lax.fori_loop(0, nx, row_step, 0, unroll=2)
        for q in stages[c]:
            out_copies[q].start()
    disp_copy.wait()
    for copy in out_copies:
        copy.wait()


def finish(parts, scal, force, image, back_f, back_q, own, slot_hot, hot_turned, turned, read):
    hbm = pl.BlockSpec(memory_space=pltpu.HBM)
    vmem = pl.BlockSpec(memory_space=pltpu.VMEM)
    records = own.shape[1]
    dma = pltpu.SemaphoreType.DMA
    return pl.pallas_call(
        functools.partial(finish_kernel, parts),
        in_specs=[vmem] * 10,
        out_specs=[hbm, hbm],
        out_shape=[
            jax.ShapeDtypeStruct(read.shape, F32),
            jax.ShapeDtypeStruct(force.shape, F32),
        ],
        scratch_shapes=[
            pltpu.VMEM(read.shape, F32),
            pltpu.VMEM((3,) + read.shape[1:], F32),
            pltpu.VMEM((8, records), F32),
            pltpu.VMEM(force.shape, F32),
            dma((20,)),
        ],
        compiler_params=pltpu.CompilerParams(vmem_limit_bytes=24 * 2**20),
        name="finish",
    )(scal, force, image, back_f, back_q, own, slot_hot, hot_turned, turned, read)


def per_device(
    grid, populations, mass, modulus, cell_live, stiff_ref, rec_block, rec_owner, rec_node,
    rbf_weight,
):
    devices = grid[0] * grid[1]
    records = rec_block.shape[0]
    capacity = 2 * records // devices
    parts = -(-capacity // LANES)
    blk = rec_block.reshape(1, records)
    own = rec_owner.reshape(1, records)
    node = rec_node.reshape(1, records)
    operands = [
        pltpu.with_memory_space_constraint(a, pltpu.HBM)
        for a in (stiff_ref, populations, rbf_weight, blk, own, node, modulus, cell_live, mass)
    ]
    read, turned, force, image, slot_hot, hot_turned, scal, back_f, back_q, held_own = couple(
        grid, parts, *operands
    )
    return finish(
        parts, scal, force, image, back_f, back_q, held_own, slot_hot, hot_turned, turned, read
    )


def solution(mesh):
    grid = (mesh.shape["gx"], mesh.shape["gy"])
    in_specs = (
        P(None, "gx", "gy", None),
        P("gx", "gy"),
        P("gx", "gy"),
        P("gx", "gy"),
        P(),
        P(("gx", "gy")),
        P(("gx", "gy"), None),
        P(("gx", "gy")),
        P(("gx", "gy"), None),
    )
    out_specs = (P(None, "gx", "gy", None), P(None, "gx", "gy"))
    return jax.shard_map(
        functools.partial(per_device, grid), mesh=mesh, in_specs=in_specs, out_specs=out_specs,
        check_vma=False,
    )
```
